32 devices in a mesh: rep: 1 (over z), dp: 32 (over x, y, core).
Axes of the slice: x: 4, y: 4, z: 1, core: 2. Of those that a mesh axis runs over, the one named last changes fastest.
The devices are a block of a 4x4x8 slice.
Arguments:
- x: bfloat16 [32, 2048, 512], P(('rep', 'dp'))
- dy: bfloat16 [32, 2048, 512], P(('rep', 'dp'))
- w_gate: bfloat16 [2, 512, 8192], P(None, 'dp')
- w_up: bfloat16 [2, 512, 8192], P(None, 'dp')
- w_down: bfloat16 [2, 8192, 512], P(None, 'dp')
- m_w_gate: float32 [2, 512, 8192], P(None, 'dp')
- m_w_up: float32 [2, 512, 8192], P(None, 'dp')
- m_w_down: float32 [2, 8192, 512], P(None, 'dp')
- v_w_gate: float32 [2, 512, 8192], P(None, 'dp')
- v_w_up: float32 [2, 512, 8192], P(None, 'dp')
- v_w_down: float32 [2, 8192, 512], P(None, 'dp')
Outputs:
- output 1: bfloat16 [2, 512, 8192], P('rep', 'dp')
- output 2: bfloat16 [2, 512, 8192], P('rep', 'dp')
- output 3: bfloat16 [2, 8192, 512], P('rep', 'dp')
- output 4: float32 [2, 512, 8192], P('rep', 'dp')
- output 5: float32 [2, 512, 8192], P('rep', 'dp')
- output 6: float32 [2, 8192, 512], P('rep', 'dp')
- output 7: float32 [2, 512, 8192], P('rep', 'dp')
- output 8: float32 [2, 512, 8192], P('rep', 'dp')
- output 9: float32 [2, 8192, 512], P('rep', 'dp')
All inputs are finite; a program needn't handle non-finite values.
Results may differ from the reference program's by a relative error of at most 0.022.
Values are sent between devices in bfloat16 or wider.
A program may use at most 768 MiB of HBM per device.

```python
import jax
import jax.numpy as jnp
from jax import lax

SEQUENCES = 32
TOKENS = 2048
D = 512
FF = 8192
LAYERS = 2
NAMES = ("w_gate", "w_up", "w_down")
SHAPES = {"w_gate": (LAYERS, D, FF), "w_up": (LAYERS, D, FF), "w_down": (LAYERS, FF, D)}


def bump(key, n, height):
    away = (jnp.arange(n, dtype=jnp.int32) - jax.random.randint(key, (), 0, n, jnp.int32)) % n
    return jnp.where(away < n // 8, height, 1.0)


def together(key, own, strength):
    shared = jax.random.normal(key, own.shape[1:], jnp.float32)
    return (own + strength * shared) * lax.rsqrt(1 + strength * strength)


def setup_inputs(seed: int = 0, part: int = 0) -> dict:
    kx, kdy, ka, kb, kz, kf, kh, kl, *keys = jax.random.split(jax.random.key(seed), 8 + 3 * len(NAMES))
    kx, kdy, ka, kb = (jax.random.fold_in(k, part) for k in (kx, kdy, ka, kb))
    kw, km, kv = (keys[i::3] for i in range(3))
    shape = (SEQUENCES, TOKENS, D)
    much_x, much_dy = jax.random.uniform(kz, (2,), jnp.float32, 0.0, 1.0)
    loud = 2.0 ** jax.random.uniform(jax.random.fold_in(kz, 1), (), jnp.float32, -1.0, 2.0)
    layers = 2.0 ** jax.random.uniform(kl, (LAYERS, 1, 1), jnp.float32, -1.0, 1.0)
    x = together(ka, jax.random.normal(kx, shape, jnp.float32), much_x) * bump(kf, D, 4.0)
    dy = together(kb, jax.random.normal(kdy, shape, jnp.float32), much_dy)
    drawn = {"x": x.astype(jnp.bfloat16), "dy": (loud * dy * (SEQUENCES * TOKENS) ** -0.5).astype(jnp.bfloat16)}
    for key, name in zip(kw, NAMES, strict=True):
        w = jax.random.normal(key, SHAPES[name], jnp.float32) * SHAPES[name][1] ** -0.5
        drawn[name] = (w * {"w_gate": 1.0, "w_up": bump(kh, FF, 4.0), "w_down": layers}[name]).astype(jnp.bfloat16)
    for key, name in zip(km, NAMES, strict=True):
        drawn[f"m_{name}"] = 0.1 * jax.random.normal(key, SHAPES[name], jnp.float32)
    for key, name in zip(kv, NAMES, strict=True):
        drawn[f"v_{name}"] = jax.random.uniform(key, SHAPES[name], jnp.float32, 0.005, 0.015)
    return drawn


def matmul(a, w):
    return jnp.dot(a, w, preferred_element_type=jnp.float32).astype(jnp.bfloat16)


def normed(h):
    wide = h.astype(jnp.float32)
    scale = lax.rsqrt(jnp.mean(wide**2, -1, keepdims=True) + 1e-6)
    return (wide * scale).astype(jnp.bfloat16)


def layer(h, w):
    a = normed(h)
    gate = jnp.dot(a, w["w_gate"], preferred_element_type=jnp.float32)
    up = jnp.dot(a, w["w_up"], preferred_element_type=jnp.float32)
    return h + matmul((jax.nn.silu(gate) * up).astype(jnp.bfloat16), w["w_down"])


def adamw(w, m, v, g):
    m = 0.9 * m + 0.1 * g
    v = 0.95 * v + 0.05 * g * g
    step = m * lax.rsqrt(v + 1e-8) + 0.1 * w
    return (w - 0.02 * step).astype(jnp.bfloat16), m, v


def clipped(gradients, sum_of_squares, count):
    factor = jnp.minimum(1.0, 0.5 * lax.rsqrt(sum_of_squares / count + 1e-30))
    return [g * factor for g in gradients]


def stack(weights, h):
    return lax.scan(lambda h, w: (layer(h, w), None), h, weights)[0]


def reference(x, dy, w_gate, w_up, w_down, m_w_gate, m_w_up, m_w_down, v_w_gate, v_w_up, v_w_down):
    weights = dict(zip(NAMES, (w_gate, w_up, w_down), strict=True))

    def take(so_far, sequence):
        h, by_y = sequence
        _, back = jax.vjp(lambda w: stack(w, h), weights)
        return jax.tree.map(lambda total, term: total + term.astype(jnp.float32), so_far, back(by_y)[0]), None

    none_yet = {name: jnp.zeros(w.shape, jnp.float32) for name, w in weights.items()}
    by_weights, _ = lax.scan(take, none_yet, (x, dy))
    gradients = [by_weights[name].astype(jnp.bfloat16).astype(jnp.float32) for name in NAMES]
    gradients = clipped(gradients, sum(jnp.sum(g * g) for g in gradients), sum(g.size for g in gradients))
    new = [
        adamw(w.astype(jnp.float32), m, v, g)
        for w, m, v, g in zip((w_gate, w_up, w_down), (m_w_gate, m_w_up, m_w_down), (v_w_gate, v_w_up, v_w_down), gradients, strict=True)
    ]
    return tuple(one[which] for which in range(3) for one in new)
```

```python
import functools
import math

import jax
import jax.numpy as jnp
from jax import lax
from jax.experimental import pallas as pl
from jax.experimental.pallas import tpu as pltpu
from jax.sharding import PartitionSpec as P

F32, BF16 = jnp.float32, jnp.bfloat16
MESH = pl.DeviceIdType.MESH
ANY = pl.BlockSpec(memory_space=pl.ANY)
VMEM_LIMIT = 63 * 1024 * 1024
LANES = 128
SUB_ROWS, SUB_COLS, SLICE = 512, 256, 32


def dot(a, b):
    return jnp.dot(a, b, preferred_element_type=F32)


def dot_t(a, b):
    return lax.dot_general(a, b, (((1,), (1,)), ((), ())), preferred_element_type=F32)


def aligned(start, size):
    return pl.ds(pl.multiple_of(start, size), size)


def normed(h):
    wide = h.astype(F32)
    return (wide * lax.rsqrt(jnp.mean(wide * wide, -1, keepdims=True) + 1e-6)).astype(BF16)


def normed_back(h, by_a):
    wide = h.astype(F32)
    scale = lax.rsqrt(jnp.mean(wide * wide, -1, keepdims=True) + 1e-6)
    inner = jnp.mean(by_a * wide, -1, keepdims=True)
    return (by_a * scale - wide * (scale * scale * scale * inner)).astype(BF16)


class Place:
    def __init__(self, n):
        self.side = math.isqrt(n // 2)
        assert self.side == 4 and self.side * self.side * 2 == n, n
        self.me = lax.axis_index("dp")
        self.k = lax.rem(self.me, 2)
        chip = self.me // 2
        x, y = chip // self.side, lax.rem(chip, self.side)
        self.pa = jnp.where(self.k == 0, x, y)
        self.pb = jnp.where(self.k == 0, y, x)
        self.partner = chip * 2 + 1 - self.k

    def chip(self, a, b):
        a, b = lax.rem(self.pa + a + self.side, self.side), lax.rem(self.pb + b + self.side, self.side)
        return self.at(a, b)

    def at(self, a, b):
        return jnp.where(self.k == 0, a * self.side + b, b * self.side + a)

    def core(self, a, b):
        return self.chip(a, b) * 2 + self.k

    def neighbours(self):
        return self.core(1, 0), self.core(-1, 0), self.core(0, 1), self.core(0, -1), self.partner


def greet(place):
    barrier = pltpu.get_barrier_semaphore()
    for other in place.neighbours():
        pl.semaphore_signal(barrier, inc=1, device_id={"dp": other}, device_id_type=MESH)
    pl.semaphore_wait(barrier, len(place.neighbours()))


def remote(src, dst, send, recv, other):
    return pltpu.make_async_remote_copy(
        src_ref=src, dst_ref=dst, send_sem=send, recv_sem=recv, device_id={"dp": other}, device_id_type=MESH
    )


def gather_tick(place, tau, total, sems, own, buf):
    own_sem, send, recv = sems
    up_a, down_a, up_b, down_b, partner = place.neighbours()
    k, side = place.k, place.side
    half = own.shape[1] // 2
    low, high = pl.ds(0, half), pl.ds(half, half)
    slots = own_sem.shape[0]

    def stage(number, body):
        n = tau - 2 * number
        pl.when((n >= 0) & (n < total))(lambda: body(n, lax.rem(n, slots)))

    def two(n, s, base, src_up, src_down, up, down):
        return (
            remote(src_up, src_up, send.at[s, base], recv.at[s, base], up),
            remote(src_down, src_down, send.at[s, base + 1], recv.at[s, base + 1], down),
        )

    here = place.chip(0, 0)

    def own_copies(n, s):
        src = own.at[n]
        dst = buf.at[n, here, k]
        return (
            remote(src, dst, send.at[s, 0], recv.at[s, 0], up_a),
            remote(src, dst, send.at[s, 1], recv.at[s, 1], down_a),
        )

    def along_a(n, s):
        return two(n, s, 2, buf.at[n, place.chip(-1, 0), k, low], buf.at[n, place.chip(1, 0), k, high], up_a, down_a)

    def along_b(n, s):
        cps = []
        for a in range(side):
            block = buf.at[n, place.chip(a, 0), k]
            cps += two(n, s, 4, block, block, up_b, down_b)
        return cps

    def along_b2(n, s):
        cps = []
        for a in range(side):
            cps += two(n, s, 6, buf.at[n, place.chip(a, -1), k, low], buf.at[n, place.chip(a, 1), k, high], up_b, down_b)
        return cps

    def across(n, s):
        plane = buf.at[n, :, k]
        return remote(plane, plane, send.at[s, 8], recv.at[s, 8], partner)

    def wait_both(n, s, base, size):
        for d in range(2):
            for sem in (send, recv):
                pltpu.make_async_copy(size(n), size(n), sem.at[s, base + d]).wait()

    one = lambda n: buf.at[n, 0, 0]
    one_half = lambda n: buf.at[n, 0, 0, low]
    four = lambda n: buf.at[n, pl.ds(0, side), 0]
    four_half = lambda n: buf.at[n, pl.ds(0, side), 0, low]

    def stage0(n, s):
        for cp in own_copies(n, s):
            cp.start()
        pltpu.make_async_copy(own.at[n], buf.at[n, here, k], own_sem.at[s]).start()

    def stage1(n, s):
        wait_both(n, s, 0, one)
        for cp in along_a(n, s):
            cp.start()
        pltpu.make_async_copy(own.at[n], buf.at[n, here, k], own_sem.at[s]).wait()

    def stage2(n, s):
        wait_both(n, s, 2, one_half)
        for cp in along_b(n, s):
            cp.start()

    def stage3(n, s):
        wait_both(n, s, 4, four)
        for cp in along_b2(n, s):
            cp.start()

    def stage4(n, s):
        wait_both(n, s, 6, four_half)
        across(n, s).start()

    def stage5(n, s):
        across(n, s).wait()

    for number, body in enumerate((stage0, stage1, stage2, stage3, stage4, stage5)):
        stage(number, body)


GATHER_DEPTH = 10


def first_kernel(
    n_dev, x_h, dy_h, wg_h, wu_h, wd_h,
    buf_h, p_h, grad_h, dh_h,
    own, h, a, aT, dy, dyT, acc, pbuf, guv, wdv, wdc, gout, dout,
    own_sem, send, recv, in_sem, gu_sem, wdv_sem, wdc_sem, p_sem, out_sem, dout_sem,
):
    place = Place(n_dev)
    layers, rows_g, ff = wg_h.shape
    rows_d = wd_h.shape[1]
    tokens, d = x_h.shape
    blocks, quarters = 2, 4
    chips = n_dev // 2
    gu = own.shape[2]
    per = gu // LANES
    units = ff // gu
    halves = rows_d // LANES
    per_half = units // halves
    unit_rows = own.shape[1]
    downs = rows_d // unit_rows
    per_down = downs // halves
    assert units == 2 * downs and halves == 2
    total = layers * (units + downs)
    first = units + downs
    slots = pbuf.shape[0]

    def at_gu0(u):
        return 3 * (u // 2) + lax.rem(u, 2)

    def at_d0(q):
        return 3 * q + 2

    def at_gu1(u):
        return first + (per_down + per_half) * (u // per_half) + per_down + lax.rem(u, per_half)

    def at_d1(q):
        return first + (per_down + per_half) * (q // per_down) + lax.rem(q, per_down)

    def own_pieces(layer, u, n):
        half_no, group = u // per_half, lax.rem(u, per_half)
        for j in range(per):
            cols = aligned((group * per + j) * rows_d + half_no * LANES, LANES)
            for w, r in ((wg_h, 0), (wu_h, rows_g)):
                yield pltpu.make_async_copy(
                    w.at[layer, :, cols], own.at[n, pl.ds(r, rows_g), pl.ds(j * LANES, LANES)], in_sem.at[4]
                )

    def own_down(layer, q, n):
        return pltpu.make_async_copy(wd_h.at[layer, aligned(q * unit_rows, unit_rows)], own.at[n], in_sem.at[4])

    loads = [(x_h, h), (dy_h, dy)]
    for i, (src, dst) in enumerate(loads):
        pltpu.make_async_copy(src, dst, in_sem.at[i]).start()
    for layer, at_gu, at_d in ((0, at_gu0, at_d0), (1, at_gu1, at_d1)):

        @pl.loop(0, units)
        def _(u):
            for cp in own_pieces(layer, u, at_gu(u)):
                cp.start()

        @pl.loop(0, downs)
        def _(q):
            own_down(layer, q, at_d(q)).start()

    greet(place)
    pltpu.make_async_copy(own, own, in_sem.at[4]).wait()

    def tick(tau):
        gather_tick(place, tau, total, (own_sem, send, recv), own, buf_h)

    def gu_load(n, slot):
        return pltpu.make_async_copy(buf_h.at[n], guv.at[slot], gu_sem.at[slot])

    def wdv_load(q):
        half_no, part = q // per_down, lax.rem(q, per_down)
        return pltpu.make_async_copy(
            buf_h.at[at_d0(q)], wdv.at[half_no, :, :, aligned(part * unit_rows, unit_rows)], wdv_sem
        )

    def gate_up(slot):
        w = guv[slot].reshape(n_dev, unit_rows, gu)
        return w[:, :rows_g].reshape(d, gu), w[:, rows_g:].reshape(d, gu)

    def p_store(u):
        slot = lax.rem(u, slots)
        return pltpu.make_async_copy(pbuf.at[slot], p_h.at[u], p_sem.at[slot])

    def hidden(u):
        slot = lax.rem(u, 2)
        out = lax.rem(u, slots)
        gu_load(at_gu0(u), slot).wait()

        @pl.when(u >= slots)
        def _():
            p_store(u - slots).wait()

        @pl.loop(0, blocks)
        def _(t):
            tb = tokens // blocks
            wg, wu = gate_up(slot)
            for r in range(0, tb, SUB_ROWS):
                at = a[aligned(t * tb + r, SUB_ROWS)]
                for col in range(0, gu, SUB_COLS):
                    cols = slice(col, col + SUB_COLS)
                    g_all, up_all = dot(at, wg[:, cols]), dot(at, wu[:, cols])
                    for q in range(0, SUB_ROWS, SLICE):
                        g, up = g_all[q : q + SLICE], up_all[q : q + SLICE]
                        pbuf[out, aligned(t * tb + r + q, SLICE), cols] = (g * (1.0 / (1.0 + jnp.exp(-g))) * up).astype(BF16)

        p_store(u).start()

    def down(half_no, t):
        rows = aligned(t * (tokens // quarters), tokens // quarters)
        total_ = None
        for j in range(per_half):
            w = wdv[half_no, pl.ds(j * per // 2, per // 2)].reshape(gu, d)
            term = dot(pbuf[(half_no * per_half + j) % slots, rows], w)
            total_ = term if total_ is None else total_ + term
        if half_no == 0:
            acc[rows] = total_
        else:
            acc[rows] += total_

    for i, (src, dst) in enumerate(loads):
        pltpu.make_async_copy(src, dst, in_sem.at[i]).wait()

    @pl.loop(0, tokens // 256)
    def _(t):
        rows = aligned(t * 256, 256)
        a[rows] = normed(h[rows])
        dyT[:, rows] = dy[rows].astype(F32).T.astype(BF16)

    @pl.loop(0, first + GATHER_DEPTH + 1)
    def _(tau):
        tick(tau)
        done = tau - GATHER_DEPTH
        kind, r = lax.rem(done, 3), done // 3

        @pl.when((done >= 0) & (done < first))
        def _():
            @pl.when(kind < 2)
            def _():
                gu_load(done, kind).start()

            @pl.when(kind == 2)
            def _():
                wdv_load(r).start()

        n = done - 1
        kind_n, r_n = lax.rem(n, 3), n // 3

        @pl.when(n >= 0)
        def _():
            @pl.when(kind_n < 2)
            def _():
                hidden(2 * r_n + kind_n)

            @pl.when(kind_n == 2)
            def _():
                wdv_load(r_n).wait()

                @pl.when((r_n >= per_down) & (r_n < per_down + 2))
                def _():
                    @pl.loop(0, quarters // 2)
                    def _(t):
                        down(0, (r_n - per_down) * (quarters // 2) + t)

    after = first + GATHER_DEPTH + 1

    @pl.loop(0, quarters)
    def _(t):
        tick(after + t)
        down(1, t)

    after += quarters

    def weights_of(u, slot):
        half_no, group = u // per_half, lax.rem(u, per_half)
        yield gu_load(at_gu1(u), slot)
        for part in range(per_down):
            yield pltpu.make_async_copy(
                buf_h.at[at_d1(half_no * per_down + part), aligned(group * (per // 2), per // 2)],
                wdc.at[slot, :, :, pl.ds(part * unit_rows, unit_rows)],
                wdc_sem.at[slot, part],
            )

    for cp in weights_of(jnp.int32(0), jnp.int32(0)):
        cp.start()
    for i in range(slots):
        p_store(units - slots + i).wait()

    @pl.loop(0, tokens // 256)
    def _(t):
        rows = aligned(t * 256, 256)
        h1 = (h[rows].astype(F32) + acc[rows].astype(BF16).astype(F32)).astype(BF16)
        h[rows] = h1
        a1 = normed(h1)
        a[rows] = a1
        aT[:, rows] = a1.astype(F32).T.astype(BF16)
        acc[rows] = jnp.zeros((256, d), F32)

    def body(c, t, now, before, grads):
        backward_body(
            c, t, now, before, grads, blocks, a, aT, dy, dyT, acc,
            pbuf.at[pl.ds(0, 2)], pbuf.at[pl.ds(2, 2)], pbuf.at[pl.ds(4, 2)],
            gate_up, lambda slot: wdc[slot].reshape(gu, d), gout, dout,
        )

    def flush(c):
        slot = lax.rem(c, 2)
        half_no, group = c // per_half, lax.rem(c, per_half)
        yield pltpu.make_async_copy(gout.at[slot], grad_h.at[1, c], out_sem.at[slot])
        for part in range(per_down):
            yield pltpu.make_async_copy(
                dout.at[slot, :, :, pl.ds(part * unit_rows, unit_rows)],
                grad_h.at[1, units + half_no * per_down + part, aligned(group * (per // 2), per // 2)],
                dout_sem.at[slot, part],
            )

    def chunk_ticks(c):
        @pl.when(after + 2 * c < total + GATHER_DEPTH)
        def _():
            tick(after + 2 * c)
            tick(after + 2 * c + 1)

    backward_loop(units, blocks, body, weights_of, flush, chunk_ticks)

    @pl.loop(0, tokens // 256)
    def _(t):
        rows = aligned(t * 256, 256)
        by_a = acc[rows].astype(BF16).astype(F32)
        back = normed_back(h[rows], by_a)
        a[rows] = (dy[rows].astype(F32) + back.astype(F32)).astype(BF16)

    cp = pltpu.make_async_copy(a, dh_h, in_sem.at[0])
    cp.start()
    cp.wait()


def backward_body(c, t, now, before, grads, blocks, a, aT, by, byT, acc, ps, dg, du, gate_up, down, gout, dout):
    slot = lax.rem(c, 2)
    other = 1 - slot
    tokens, d = a.shape
    tb = tokens // blocks
    part = d // blocks
    fill = []

    def states(i):
        slot_b = jnp.where(t == 0, other, slot)
        rows_b = aligned(lax.rem(t + blocks - 1, blocks) * tb + i * (tb // 2), tb // 2)
        wg, wu = gate_up(slot_b)
        acc[rows_b] += dot_t(dg[slot_b, rows_b], wg) + dot_t(du[slot_b, rows_b], wu)

    def weights(i):
        m = aligned(t * part, part)
        if i == 2:
            dout[other, :, :, :, m] = dot(byT[m], ps[other]).T.astype(BF16).reshape(dout.shape[1:4] + (part,))
            return
        rows_g = gout.shape[3] // 2
        chips = part // rows_g // 2
        grad = dot(aT[m], (dg, du)[i][other]).astype(BF16)
        gout[other, aligned(t * chips, chips), :, pl.ds(i * rows_g, rows_g)] = grad.reshape(chips, 2, rows_g, -1)

    if before and acc is not None:
        fill += [functools.partial(states, i) for i in range(2)]
    if grads:
        fill += [functools.partial(weights, i) for i in range(3 if ps is not None else 2)]
    if not now:
        for piece in fill:
            piece()
        return
    wg, wu = gate_up(slot)
    wd = down(slot)
    gu = wg.shape[1]
    tiles = [(r, col) for r in range(0, tb, SUB_ROWS) for col in range(0, gu, SUB_COLS)]
    done = 0
    for i, (r, col) in enumerate(tiles):
        cols = slice(col, col + SUB_COLS)
        rows = aligned(t * tb + r, SUB_ROWS)
        at = a[rows]
        g_all, up_all = dot(at, wg[:, cols]), dot(at, wu[:, cols])
        dp_all = dot_t(by[rows], wd[cols])
        while done < len(fill) * (i + 1) // len(tiles):
            fill[done]()
            done += 1
        for q in range(0, SUB_ROWS, SLICE):
            g, up, dp = g_all[q : q + SLICE], up_all[q : q + SLICE], dp_all[q : q + SLICE].astype(BF16).astype(F32)
            sig = 1.0 / (1.0 + jnp.exp(-g))
            silu = g * sig
            out = aligned(t * tb + r + q, SLICE)
            if ps is not None:
                ps[slot, out, cols] = (silu * up).astype(BF16)
            du[slot, out, cols] = (dp * silu).astype(BF16)
            dg[slot, out, cols] = (dp * up * (sig + silu * (1.0 - sig))).astype(BF16)


def backward_loop(units, blocks, body, weights_of, flush, ticks, each=lambda c, t: None):
    zero = jnp.int32(0)

    def arrive(c):
        for cp in weights_of(c, lax.rem(c, 2)):
            cp.wait()

    def prefetch(c):
        @pl.when(c + 1 < units)
        def _():
            for cp in weights_of(c + 1, lax.rem(c + 1, 2)):
                cp.start()

    def start(c):
        for cp in flush(c):
            cp.start()

    def wait(c):
        for cp in flush(c):
            cp.wait()

    arrive(zero)
    ticks(zero)
    each(zero, zero)
    body(zero, zero, True, False, False)
    prefetch(zero)

    @pl.loop(1, blocks)
    def _(t):
        each(zero, t)
        body(zero, t, True, True, False)

    @pl.loop(1, units)
    def _(c):
        arrive(c)
        ticks(c)
        each(c, zero)
        body(c, zero, True, True, True)
        prefetch(c)
        pl.when(c > 1)(lambda: wait(c - 2))

        @pl.loop(1, blocks)
        def _(t):
            each(c, t)
            body(c, t, True, True, True)

        start(c - 1)

    last = jnp.int32(units)
    each(last, zero)
    body(last, zero, False, True, True)
    wait(last - 2)

    @pl.loop(1, blocks)
    def _(t):
        each(last, t)
        body(last, t, False, False, True)

    start(last - 1)
    wait(last - 1)


SCATTER_STAGES = 7
SCATTER_AT = (0, 1, 3, 5, 7, 9, 11)
SCATTER_DEPTH = SCATTER_AT[-1]
CREDIT = 2


def scatter_tick(place, tau, issued, source, target, refs):
    grad, got0, out1, got1, out2, got2, mid, out3, got3, out4, got4, fin, squares, load_sem, send, recv, fin_sem, credit = refs
    up_a, down_a, up_b, down_b, partner = place.neighbours()
    neighbours = place.neighbours()
    k, side = place.k, place.side
    half = grad.shape[3] // 2
    low, high = pl.ds(0, half), pl.ds(half, half)
    big, small = grad.shape[0], send.shape[0]

    def f(x):
        return x.astype(F32)

    @pl.when(tau >= CREDIT)
    def _():
        for i in range(len(neighbours)):
            pl.semaphore_wait(credit.at[i], 1)

    def load(b, n):
        return pltpu.make_async_copy(source(n), grad.at[b], load_sem.at[b])

    def across(b, s):
        return (remote(grad.at[b, :, 1 - k], got0.at[b], send.at[s, 0], recv.at[s, 0], partner),)

    def pair(out, got, s, base, up, down):
        return (
            remote(out.at[s, 0], got.at[s, 0], send.at[s, base], recv.at[s, base], up),
            remote(out.at[s, 1], got.at[s, 1], send.at[s, base + 1], recv.at[s, base + 1], down),
        )

    def along_b(s):
        return pair(out1, got1, s, 1, up_b, down_b)

    def along_b2(s):
        return pair(out2, got2, s, 3, up_b, down_b)

    def along_a(s):
        return pair(out3, got3, s, 5, up_a, down_a)

    def along_a2(s):
        return pair(out4, got4, s, 7, up_a, down_a)

    def store(s, n):
        return pltpu.make_async_copy(fin.at[s], target(n), fin_sem.at[s])

    def stage0(b, s, n):
        load(b, n).start()

    def stage1(b, s, n):
        load(b, n).wait()
        for cp in across(b, s):
            cp.start()

    def stage2(b, s, n):
        for cp in across(b, s):
            cp.wait()
        for i in range(side):
            chip = place.at(i, lax.rem(place.pb + 2, side))
            total = f(grad[b, chip, k]) + f(got0[b, chip])
            out1[s, 0, i] = total[:half].astype(BF16)
            out1[s, 1, i] = total[half:].astype(BF16)
        for cp in along_b(s):
            cp.start()

    def stage3(b, s, n):
        for cp in along_b(s):
            cp.wait()
        for i in range(side):
            for way, step in ((0, 1), (1, side - 1)):
                chip = place.at(i, lax.rem(place.pb + step, side))
                total = f(grad[b, chip, k]) + f(got0[b, chip])
                whole = pl.ds(half * way, half)
                rest = pl.ds(half * (1 - way), half)
                out2[s, way, i, whole] = (total[half * way : half * way + half] + f(got1[s, way, i])).astype(BF16)
                out2[s, way, i, rest] = total[half * (1 - way) : half * (2 - way)].astype(BF16)
        for cp in along_b2(s):
            cp.start()

    def stage4(b, s, n):
        for cp in along_b2(s):
            cp.wait()
        for i in range(side):
            chip = place.at(i, place.pb)
            mid[b, i] = f(grad[b, chip, k]) + f(got0[b, chip]) + f(got2[s, 0, i]) + f(got2[s, 1, i])
        far = mid[b, lax.rem(place.pa + 2, side)]
        out3[s, 0] = far[:half].astype(BF16)
        out3[s, 1] = far[half:].astype(BF16)
        for cp in along_a(s):
            cp.start()

    def stage5(b, s, n):
        for cp in along_a(s):
            cp.wait()
        for way, step in ((0, 1), (1, side - 1)):
            total = mid[b, lax.rem(place.pa + step, side)]
            whole = pl.ds(half * way, half)
            rest = pl.ds(half * (1 - way), half)
            out4[s, way, whole] = (total[half * way : half * way + half] + f(got3[s, way])).astype(BF16)
            out4[s, way, rest] = total[half * (1 - way) : half * (2 - way)].astype(BF16)
        for cp in along_a2(s):
            cp.start()

    def stage6(b, s, n):
        for cp in along_a2(s):
            cp.wait()
        result = (mid[b, place.pa] + f(got4[s, 0]) + f(got4[s, 1])).astype(BF16)
        fin[s] = result
        squares[...] += f(result) * f(result)
        cp = store(s, n)
        cp.start()
        cp.wait()

    for after, body in zip(SCATTER_AT, (stage0, stage1, stage2, stage3, stage4, stage5, stage6), strict=True):
        began = tau - after
        here, n = issued(began)
        pl.when((began >= 0) & here)(functools.partial(body, lax.rem(began, big), lax.rem(began, small), n))

    for i, (other, seen_as) in enumerate(zip(neighbours, (1, 0, 3, 2, 4), strict=True)):
        pl.semaphore_signal(credit.at[seen_as], inc=1, device_id={"dp": other}, device_id_type=MESH)


def second_kernel(
    n_dev, x_h, by_h, buf_h, p_h, _,
    grads_h, fin_h, total_o,
    a, aT, by, byT, dg, du, guv, wdc, gout, dout, pv,
    grad, got0, out1, got1, out2, got2, mid, out3, got3, out4, got4, fin, squares, mine, theirs,
    in_sem, gu_sem, wdc_sem, p_sem, out_sem, dout_sem,
    load_sem, send, recv, fin_sem, credit, sum_send, sum_recv,
):
    place = Place(n_dev)
    tokens, d = x_h.shape
    units, _, gu = p_h.shape
    per = gu // LANES
    halves = 2
    per_half = units // halves
    unit_rows = grads_h.shape[4]
    downs = grads_h.shape[1] - units
    per_down = downs // halves
    total = units + downs
    blocks = 2

    for i, (src, dst) in enumerate(((x_h, a), (by_h, by))):
        pltpu.make_async_copy(src, dst, in_sem.at[i]).start()
    greet(place)

    def at_gu0(u):
        return 3 * (u // 2) + lax.rem(u, 2)

    def at_d0(q):
        return 3 * q + 2

    def p_load(u):
        slot = lax.rem(u, 2)
        return pltpu.make_async_copy(p_h.at[u], pv.at[slot], p_sem.at[slot])

    p_load(jnp.int32(0)).start()
    for i, (src, dst) in enumerate(((x_h, a), (by_h, by))):
        pltpu.make_async_copy(src, dst, in_sem.at[i]).wait()

    @pl.loop(0, tokens // 256)
    def _(t):
        rows = aligned(t * 256, 256)
        a0 = normed(a[rows])
        a[rows] = a0
        aT[:, rows] = a0.astype(F32).T.astype(BF16)
        byT[:, rows] = by[rows].astype(F32).T.astype(BF16)

    squares[...] = jnp.zeros_like(squares)

    backlog = total + downs

    def issued(tau):
        chunk, t = tau // 4 - units // 4, lax.rem(tau, 4)
        early = tau < units + 8
        n = jnp.where(early, 3 * (tau // 4) + t, 3 * (units // 4 + 2) + 2 * (chunk - 2) + t)
        u = chunk - 2
        made = (t == 3) & (early == False) & (u < units)
        here = jnp.where(early, t != 3, (t < 2) & (n < backlog))
        return here | made, jnp.where(made, backlog + u, n)

    ticks = units + 4 * (units + 2) + SCATTER_DEPTH

    def source_of(n):
        layer1 = n < total
        return layer1, jnp.where(layer1, n, jnp.where(n < backlog, n - total + units, n - backlog))

    refs = (grad, got0, out1, got1, out2, got2, mid, out3, got3, out4, got4, fin, squares, load_sem, send, recv, fin_sem, credit)

    def tick(tau):
        def source(n):
            layer1, i = source_of(n)
            return grads_h.at[layer1.astype(jnp.int32), i]

        def target(n):
            layer1, i = source_of(n)
            return fin_h.at[layer1.astype(jnp.int32), i]

        scatter_tick(place, tau, issued, source, target, refs)

    def gate_up(slot):
        w = guv[slot].reshape(n_dev, unit_rows, gu)
        return w[:, : unit_rows // 2].reshape(d, gu), w[:, unit_rows // 2 :].reshape(d, gu)

    def split(c):
        return c // per_half, lax.rem(c, per_half)

    def weights_of(u, slot):
        half_no, group = split(u)
        yield pltpu.make_async_copy(buf_h.at[at_gu0(u)], guv.at[slot], gu_sem.at[slot])
        for part in range(per_down):
            yield pltpu.make_async_copy(
                buf_h.at[at_d0(half_no * per_down + part), aligned(group * (per // 2), per // 2)],
                wdc.at[slot, :, :, pl.ds(part * unit_rows, unit_rows)],
                wdc_sem.at[slot, part],
            )

    def down_store(c):
        slot = lax.rem(c, 2)
        half_no, group = split(c)
        for part in range(per_down):
            yield pltpu.make_async_copy(
                dout.at[slot, :, :, pl.ds(part * unit_rows, unit_rows)],
                grads_h.at[0, units + half_no * per_down + part, aligned(group * (per // 2), per // 2)],
                dout_sem.at[slot, part],
            )

    def flush(c):
        slot = lax.rem(c, 2)
        yield pltpu.make_async_copy(gout.at[slot], grads_h.at[0, c], out_sem.at[slot])

    for cp in weights_of(jnp.int32(0), jnp.int32(0)):
        cp.start()

    @pl.loop(0, units)
    def _(u):
        slot = lax.rem(u, 2)
        p_load(u).wait()

        @pl.when(u + 1 < units)
        def _():
            p_load(u + 1).start()

        tick(u)

        @pl.when(u > 1)
        def _():
            for cp in down_store(u - 2):
                cp.wait()

        for r in range(0, d, d // 2):
            m = pl.ds(r, d // 2)
            dout[slot, :, :, :, m] = dot(byT[m], pv[slot]).T.astype(BF16).reshape(dout.shape[1:4] + (d // 2,))
        for cp in down_store(u):
            cp.start()

    for u in (units - 2, units - 1):
        for cp in down_store(jnp.int32(u)):
            cp.wait()

    def body(c, t, now, before, grads):
        backward_body(
            c, t, now, before, grads, blocks, a, aT, by, byT, None, None, dg, du,
            gate_up, lambda slot: wdc[slot].reshape(gu, d), gout, None,
        )

    def each(c, t):
        first = units + 4 * c + 2 * t
        tick(first)
        tick(first + 1)

    backward_loop(units, blocks, body, weights_of, flush, lambda c: None, each)

    @pl.loop(units + 4 * (units + 1), ticks)
    def _(tau):
        tick(tau)

    for i in range(len(place.neighbours())):
        pl.semaphore_wait(credit.at[i], CREDIT)

    up_a, down_a, up_b, down_b, partner = place.neighbours()
    others = [partner]
    for p, up, down in ((place.pa, up_a, down_a), (place.pb, up_b, down_b)):
        even = lax.rem(p, 2) == 0
        others += [jnp.where(even, up, down), jnp.where(even, down, up)]
    so_far = jnp.full(mine.shape[1:], jnp.sum(squares[...]), F32)
    for i, other in enumerate(others):
        mine[i] = so_far
        cp = remote(mine.at[i], theirs.at[i], sum_send.at[i], sum_recv.at[i], other)
        cp.start()
        cp.wait()
        so_far = so_far + theirs[i]
    total_o[...] = so_far


def adamw(w, m, v, g):
    m = 0.9 * m + 0.1 * g
    v = 0.95 * v + 0.05 * g * g
    step = m * lax.rsqrt(v + 1e-8) + 0.1 * w
    return (w - 0.02 * step).astype(BF16), m, v


def solution(mesh):
    n_dev = mesh.shape["dp"]

    def step(x, dy, *arrays):
        weights, m, v = (arrays[i : i + 3] for i in (0, 3, 6))
        x, dy = x[0], dy[0]
        w_gate, w_up, w_down = weights
        layers, rows_g, ff = w_gate.shape
        assert layers == 2
        rows_d, d = w_down.shape[1:]
        tokens = x.shape[0]
        chips = n_dev // 2
        halves = rows_d // LANES
        gu = d
        units, unit_rows = ff // gu, 2 * rows_g
        downs = rows_d // unit_rows
        per = gu // LANES
        total = units + downs
        vmem, dma = pltpu.VMEM, pltpu.SemaphoreType.DMA
        shape = jax.ShapeDtypeStruct
        unit = (chips, 2, unit_rows, gu)
        states = (tokens, d)

        buf, p, grads, by = pl.pallas_call(
            functools.partial(first_kernel, n_dev),
            out_shape=(
                shape((layers * total,) + unit, BF16),
                shape((units, tokens, gu), BF16),
                shape((layers, total) + unit, BF16),
                shape(states, BF16),
            ),
            in_specs=[ANY] * 5,
            out_specs=[ANY] * 4,
            scratch_shapes=[
                vmem((layers * total, unit_rows, gu), BF16),
                vmem(states, BF16),
                vmem(states, BF16),
                vmem(states[::-1], BF16),
                vmem(states, BF16),
                vmem(states[::-1], BF16),
                vmem(states, F32),
                vmem((12, tokens, gu), BF16),
                vmem((2,) + unit, BF16),
                vmem((halves, chips, 2, LANES, d), BF16),
                vmem((2, per // 2, 2, LANES, d), BF16),
                vmem((2,) + unit, BF16),
                vmem((2, per // 2, 2, LANES, d), BF16),
                dma((8,)),
                dma((8, 9)),
                dma((8, 9)),
                dma((5,)),
                dma((2,)),
                dma,
                dma((2, downs // halves)),
                dma((12,)),
                dma((2,)),
                dma((2, downs // halves)),
            ],
            compiler_params=pltpu.CompilerParams(collective_id=0, has_side_effects=True, vmem_limit_bytes=VMEM_LIMIT),
            name="forward_backward",
        )(x, dy, w_gate, w_up, w_down)

        big, small, side = 8, 4, math.isqrt(chips)
        half_block, block = (unit_rows // 2, gu), (unit_rows, gu)
        grads, fin, squares = pl.pallas_call(
            functools.partial(second_kernel, n_dev),
            out_shape=(
                shape(grads.shape, BF16),
                shape((layers, total) + block, BF16),
                shape((8, LANES), F32),
            ),
            in_specs=[ANY] * 5,
            out_specs=[ANY, ANY, pl.BlockSpec(memory_space=vmem)],
            scratch_shapes=[
                vmem(states, BF16),
                vmem(states[::-1], BF16),
                vmem(states, BF16),
                vmem(states[::-1], BF16),
                vmem((2, tokens, gu), BF16),
                vmem((2, tokens, gu), BF16),
                vmem((2,) + unit, BF16),
                vmem((2, per // 2, 2, LANES, d), BF16),
                vmem((2,) + unit, BF16),
                vmem((2, per // 2, 2, LANES, d), BF16),
                vmem((2, tokens, gu), BF16),
                vmem((big,) + unit, BF16),
                vmem((big, chips) + block, BF16),
                vmem((small, 2, side) + half_block, BF16),
                vmem((small, 2, side) + half_block, BF16),
                vmem((small, 2, side) + block, BF16),
                vmem((small, 2, side) + block, BF16),
                vmem((big, side) + block, F32),
                vmem((small, 2) + half_block, BF16),
                vmem((small, 2) + half_block, BF16),
                vmem((small, 2) + block, BF16),
                vmem((small, 2) + block, BF16),
                vmem((small,) + block, BF16),
                vmem(block, F32),
                vmem((5, 8, LANES), F32),
                vmem((5, 8, LANES), F32),
                dma((2,)),
                dma((2,)),
                dma((2, downs // halves)),
                dma((2,)),
                dma((2,)),
                dma((2, downs // halves)),
                dma((big,)),
                dma((small, 9)),
                dma((small, 9)),
                dma((small,)),
                pltpu.SemaphoreType.REGULAR((5,)),
                dma((5,)),
                dma((5,)),
            ],
            input_output_aliases={4: 0},
            compiler_params=pltpu.CompilerParams(collective_id=1, has_side_effects=True, vmem_limit_bytes=VMEM_LIMIT),
            name="backward_scatter",
        )(x, by, buf, p, grads)

        pair = fin[:, :units].reshape(layers, halves, units // halves, 2, rows_g, per, LANES)
        pair = pair.transpose(3, 0, 4, 2, 5, 1, 6).reshape(2, layers, rows_g, ff)
        gradients = [pair[0], pair[1], fin[:, units:].reshape(layers, rows_d, d)]
        count = n_dev * sum(g.size for g in gradients)
        factor = jnp.minimum(1.0, 0.5 * lax.rsqrt(squares[0, 0] / count + 1e-30))
        new = [adamw(w.astype(F32), m, v, g.astype(F32) * factor) for w, m, v, g in zip(weights, m, v, gradients, strict=True)]
        return tuple(one[which] for which in range(3) for one in new)

    states, cut = P(("rep", "dp"), None, None), P(None, "dp", None)
    return jax.shard_map(
        step,
        mesh=mesh,
        in_specs=(states, states) + (cut,) * 9,
        out_specs=(P("rep", "dp", None),) * 9,
        check_vma=False,
    )
```

```python
import functools
import itertools
import math

import jax
import jax.numpy as jnp
from jax import lax
from jax.experimental import pallas as pl
from jax.experimental.pallas import tpu as pltpu
from jax.sharding import PartitionSpec as P

F32, BF16 = jnp.float32, jnp.bfloat16
MESH = pl.DeviceIdType.MESH
ANY = pl.BlockSpec(memory_space=pl.ANY)
VMEM_LIMIT = 63 * 1024 * 1024
LANES = 128
SUB_ROWS, SUB_COLS, SLICE = 512, 256, 32


def dot(a, b):
    return jnp.dot(a, b, preferred_element_type=F32)


def dot_t(a, b):
    return lax.dot_general(a, b, (((1,), (1,)), ((), ())), preferred_element_type=F32)


def aligned(start, size):
    return pl.ds(pl.multiple_of(start, size), size)


def div(a, b):
    return lax.div(a, jnp.int32(b))


def rem(a, b):
    return lax.rem(a, jnp.int32(b))


def where(test, a, b):
    return lax.select(test, jnp.asarray(a, jnp.int32), jnp.asarray(b, jnp.int32))


def normed(h):
    wide = h.astype(F32)
    return (wide * lax.rsqrt(jnp.mean(wide * wide, -1, keepdims=True) + 1e-6)).astype(BF16)


def normed_back(h, by_a):
    wide = h.astype(F32)
    scale = lax.rsqrt(jnp.mean(wide * wide, -1, keepdims=True) + 1e-6)
    inner = jnp.mean(by_a * wide, -1, keepdims=True)
    return (by_a * scale - wide * (scale * scale * scale * inner)).astype(BF16)


class Place:
    def __init__(self, n):
        self.side = math.isqrt(n // 2)
        assert self.side == 4 and self.side * self.side * 2 == n, n
        self.me = lax.axis_index("dp")
        self.k = rem(self.me, 2)
        chip = div(self.me, 2)
        x, y = div(chip, self.side), rem(chip, self.side)
        self.pa = where(self.k == 0, x, y)
        self.pb = where(self.k == 0, y, x)
        self.partner = chip * 2 + 1 - self.k
        self.x, self.y = x, y
        self.near = self.core(1, 0), self.core(-1, 0), self.core(0, 1), self.core(0, -1), self.partner

    def lines(self):
        side, row = self.side, 2 * self.side
        spot = self.x * 2 + self.k

        def along_x(i):
            i = rem(spot + i, row)
            return (div(i, 2) * side + self.y) * 2 + rem(i, 2)

        def along_y(i):
            return (self.x * side + rem(self.y + i, side)) * 2 + self.k

        return (spot, row, along_x), (self.y, side, along_y)

    def spot(self, a, b):
        a, b = rem(self.pa + a + self.side, self.side), rem(self.pb + b + self.side, self.side)
        return where(self.k == 0, a, b), where(self.k == 0, b, a)

    def chip(self, a, b):
        a, b = rem(self.pa + a + self.side, self.side), rem(self.pb + b + self.side, self.side)
        return self.at(a, b)

    def at(self, a, b):
        return where(self.k == 0, a * self.side + b, b * self.side + a)

    def core(self, a, b):
        return self.chip(a, b) * 2 + self.k

    def neighbours(self):
        return self.near


def greet(others):
    barrier = pltpu.get_barrier_semaphore()
    for other in others:
        pl.semaphore_signal(barrier, inc=1, device_id={"dp": other}, device_id_type=MESH)
    pl.semaphore_wait(barrier, len(others))


def remote(src, dst, send, recv, other):
    return pltpu.make_async_remote_copy(
        src_ref=src, dst_ref=dst, send_sem=send, recv_sem=recv, device_id={"dp": other}, device_id_type=MESH
    )


def gather_tick(place, tau, total, sems, own, buf):
    own_sem, send, recv = sems
    up_a, down_a, up_b, down_b, partner = place.neighbours()
    k = place.k
    half = own.shape[1] // 2
    low, high = pl.ds(0, half), pl.ds(half, half)
    slots = own_sem.shape[0]

    def stage(number, body):
        n = tau - 2 * number
        pl.when((n >= 0) & (n < total))(lambda: body(n, rem(n, slots)))

    def two(n, s, base, src_up, src_down, up, down):
        return (
            remote(src_up, src_up, send.at[s, base], recv.at[s, base], up),
            remote(src_down, src_down, send.at[s, base + 1], recv.at[s, base + 1], down),
        )

    def at(n, a, b, *rows):
        x, y = place.spot(a, b)
        return buf.at[(n, x, y, k) + rows]

    def own_copies(n, s):
        src, dst = own.at[n], at(n, 0, 0)
        return (
            remote(src, dst, send.at[s, 0], recv.at[s, 0], up_a),
            remote(src, dst, send.at[s, 1], recv.at[s, 1], down_a),
        )

    def along_a(n, s):
        return two(n, s, 2, at(n, -1, 0, low), at(n, 1, 0, high), up_a, down_a)

    def lines(n, b, rows=slice(None)):
        x, y = place.spot(0, b)
        yield from (buf.at[n, :, y, 0, rows], buf.at[n, x, :, 1, rows])

    def start_lines(s, base, ups, downs):
        for core, (src_up, src_down) in enumerate(zip(ups, downs, strict=True)):

            @pl.when(k == core)
            def _():
                for cp in two(None, s, base, src_up, src_down, up_b, down_b):
                    cp.start()

    def across(n, s):
        plane = buf.at[n, :, :, k]
        return remote(plane, plane, send.at[s, 8], recv.at[s, 8], partner)

    def wait_both(n, s, base, size):
        for d in range(2):
            for sem in (send, recv):
                pltpu.make_async_copy(size(n), size(n), sem.at[s, base + d]).wait()

    one = lambda n: buf.at[n, 0, 0, 0]
    one_half = lambda n: buf.at[n, 0, 0, 0, low]
    four = lambda n: buf.at[n, 0, :, 0]
    four_half = lambda n: buf.at[n, 0, :, 0, low]

    def stage0(n, s):
        for cp in own_copies(n, s):
            cp.start()
        pltpu.make_async_copy(own.at[n], at(n, 0, 0), own_sem.at[s]).start()

    def stage1(n, s):
        wait_both(n, s, 0, one)
        for cp in along_a(n, s):
            cp.start()
        pltpu.make_async_copy(own.at[n], at(n, 0, 0), own_sem.at[s]).wait()

    def stage2(n, s):
        wait_both(n, s, 2, one_half)
        start_lines(s, 4, lines(n, 0), lines(n, 0))

    def stage3(n, s):
        wait_both(n, s, 4, four)
        start_lines(s, 6, lines(n, -1, low), lines(n, 1, high))

    def stage4(n, s):
        wait_both(n, s, 6, four_half)
        across(n, s).start()

    def stage5(n, s):
        across(n, s).wait()

    for number, body in enumerate((stage0, stage1, stage2, stage3, stage4, stage5)):
        stage(number, body)


GATHER_DEPTH = 10


def step_kernel(
    n_dev, x_h, dy_h, wg_h, wu_h, wd_h,
    buf_h, p_h, grads_h, fin_h, total_o,
    own, h, a, by, acc, guv,
    byT, grad, got0, out1, got1, out2, got2, mid, out3, got3, out4, got4, fin, squares, rows1, rows2,
    own_sem, g_send, g_recv, in_sem, gu_sem, wd_sem, p_sem, dout_sem,
    load_sem, s_send, s_recv, fin_sem, credit, sum_send, sum_recv,
):
    place = Place(n_dev)
    layers, rows_g, ff = wg_h.shape
    rows_d = wd_h.shape[1]
    tokens, d = x_h.shape
    blocks, quarters, strip = 2, 4, 256
    chips = n_dev // 2
    unit_rows, gu = own.shape[1:]
    per = gu // LANES
    units = ff // gu
    downs = rows_d // unit_rows
    halves = rows_d // LANES
    per_half, per_down = units // halves, downs // halves
    unit = (chips, 2, unit_rows, gu)
    pairs = place.side * 2 // per
    assert halves == 2 and units == 2 * downs and layers == 2
    total = units + downs

    def split(u):
        return div(u, per_half), rem(u, per_half)

    def at_gu(layer, u):
        half_no, i = split(u)
        return layer * total + half_no * (per_half + per_down) + (layer * per_down) + i

    def at_down(layer, q):
        half_no, i = div(q, per_down), rem(q, per_down)
        return layer * total + half_no * (per_half + per_down) + ((1 - layer) * per_half) + i

    def own_pieces(layer, u, sem):
        half_no, group = split(u)
        n = at_gu(layer, u)
        for j in range(per):
            cols = aligned((group * per + j) * rows_d + half_no * LANES, LANES)
            for w, r in ((wg_h, 0), (wu_h, rows_g)):
                yield pltpu.make_async_copy(
                    w.at[layer, :, cols], own.at[n, pl.ds(r, rows_g), pl.ds(j * LANES, LANES)], in_sem.at[sem]
                )

    def own_down(layer, q, sem):
        return pltpu.make_async_copy(wd_h.at[layer, aligned(q * unit_rows, unit_rows)], own.at[at_down(layer, q)], in_sem.at[sem])

    early = 4

    @pl.loop(0, early)
    def _(u):
        for cp in own_pieces(0, u, 2):
            cp.start()

    loads = [(x_h, h), (dy_h, by)]
    for i, (src, dst) in enumerate(loads):
        pltpu.make_async_copy(src, dst, in_sem.at[i]).start()

    lines = place.lines()
    greet([other(i) for _, length, other in lines for i in range(1, length)])
    pltpu.make_async_copy(own.at[pl.ds(0, early)], own.at[pl.ds(0, early)], in_sem.at[2]).wait()

    def gather(tau):
        gather_tick(place, tau, layers * total, (own_sem, g_send, g_recv), own, buf_h)

    def gathers(first, count):
        @pl.loop(0, count)
        def _(i):
            gather(first + i)

    gathers(0, 2)
    for layer in range(layers):

        @pl.loop(early if layer == 0 else 0, units)
        def _(u):
            for cp in own_pieces(layer, u, 3):
                cp.start()

        @pl.loop(0, downs)
        def _(q):
            own_down(layer, q, 3).start()

    for i, (src, dst) in enumerate(loads):
        pltpu.make_async_copy(src, dst, in_sem.at[i]).wait()

    @pl.loop(0, tokens // strip)
    def _(t):
        rows = aligned(t * strip, strip)
        a[rows] = normed(h[rows])
        acc[rows] = jnp.zeros((strip, d), F32)

    squares[...] = jnp.zeros_like(squares)
    rest = own.at[pl.ds(early, layers * total - early)]
    pltpu.make_async_copy(rest, rest, in_sem.at[3]).wait()
    strips = tokens // strip

    def gu_load(n, slot):
        return pltpu.make_async_copy(buf_h.at[n], guv.at[slot], gu_sem.at[slot])

    def gate_up(slot):
        w = guv[slot].reshape(n_dev, unit_rows, gu)
        return w[:, :rows_g].reshape(d, gu), w[:, rows_g:].reshape(d, gu)

    def forward(pbuf, wdv):
        slots = pbuf.shape[0]

        def wd_load(q):
            part = rem(q, per_down)
            return pltpu.make_async_copy(
                buf_h.at[at_down(0, q)], wdv.at[:, :, :, aligned(part * unit_rows, unit_rows)], wd_sem.at[0, part]
            )

        def p_store(u):
            slot = rem(u, slots)
            return pltpu.make_async_copy(pbuf.at[slot], p_h.at[u], p_sem.at[slot])

        def hidden(u):
            slot, out = rem(u, 2), rem(u, slots)
            gu_load(at_gu(0, u), slot).wait()
            pl.when(u >= slots)(lambda: p_store(u - slots).wait())

            @pl.loop(0, blocks)
            def _(t):
                tb = tokens // blocks
                wg, wu = gate_up(slot)
                for r in range(0, tb, SUB_ROWS):
                    at = a[aligned(t * tb + r, SUB_ROWS)]
                    for col in range(0, gu, SUB_COLS):
                        cols = slice(col, col + SUB_COLS)
                        g_all, up_all = dot(at, wg[:, cols]), dot(at, wu[:, cols])
                        for q in range(0, SUB_ROWS, SLICE):
                            g, up = g_all[q : q + SLICE], up_all[q : q + SLICE]
                            hid = g * (1.0 / (1.0 + jnp.exp(-g))) * up
                            pbuf[out, aligned(t * tb + r + q, SLICE), cols] = hid.astype(BF16)

            p_store(u).start()

        @pl.loop(2, GATHER_DEPTH + 1)
        def _(tau):
            gather(tau)
            pl.when(tau == GATHER_DEPTH)(lambda: gu_load(0, 0).start())

            @pl.when(tau < 2 + strips)
            def _():
                rows = aligned((tau - 2) * strip, strip)
                byT[:, rows] = by[rows].astype(F32).T.astype(BF16)

        @pl.loop(0, halves)
        def _(half_no):
            now = GATHER_DEPTH + 1 + half_no * (per_half + per_down - 1 + quarters)

            @pl.loop(0, per_half)
            def _(i):
                gather(now + i)
                u = half_no * per_half + i

                @pl.when(i + 1 < per_half)
                def _():
                    gu_load(at_gu(0, u + 1), rem(u + 1, 2)).start()

                q = i - per_half + per_down

                @pl.when((q >= 0) & (half_no == 1))
                def _():
                    wd_load(per_down + q).start()

                hidden(u)

            now += per_half

            @pl.when(half_no == 0)
            def _():
                @pl.loop(0, per_down)
                def _(q):
                    pl.when(q > 0)(lambda: gather(now + q - 1))
                    wd_load(q).start()

            now += where(half_no == 0, per_down - 1, 0)
            for q in range(per_down):
                wd_load(jnp.int32(q)).wait()

            @pl.loop(0, quarters)
            def _(t):
                gather(now + t)

                @pl.when((t == quarters - 1) & (half_no == 0))
                def _():
                    gu_load(at_gu(0, per_half), 0).start()

                rows = aligned(t * (tokens // quarters), tokens // quarters)
                result = acc[rows]
                for j in range(per_half):
                    w = wdv[j // pairs, pl.ds(j % pairs * (per // 2), per // 2)].reshape(gu, d)
                    result += dot(pbuf[j, rows], w)
                acc[rows] = result

        for i in range(slots):
            p_store(jnp.int32(units - slots + i)).wait()

    pl.run_scoped(
        forward,
        pltpu.VMEM((per_half, tokens, gu), BF16),
        pltpu.VMEM((place.side, place.side, 2, LANES, d), BF16),
    )
    after = GATHER_DEPTH + 1 + per_half + (per_down - 1) + quarters + per_half + quarters

    gathers(after, 2)
    after += 2

    phase1 = blocks * (units + 1)
    phase2 = phase1 + 2
    phase3 = phase2 + units // 2
    made = 2 * blocks - 1
    early_down = blocks * (per_half + 2)
    later = downs - per_down
    last_tick = phase3 + made + 2 * (units - 1)
    windows = (
        ((early_down, early_down + 2 * per_down), (phase2, phase3 + 2 * downs)),
        ((made, made + 2 * units), (phase3 + made, last_tick + 2)),
    )
    assert blocks == 2 and phase3 == phase2 + 2 * later and phase3 % 2 == 0 and early_down % 2 == 0 and made % 2 == 1

    assert last_tick == phase3 + blocks * (units + 1) - 1

    def number(tau, odd):
        pair = where(tau < phase2, total + div(tau - made, 2), div(tau - phase3 - made, 2))
        down = where(tau < phase3, total + units + per_down + div(tau - phase2, 2), units + div(tau - phase3, 2))
        down = where(tau < phase2, total + units + div(tau - early_down, 2), down)
        return where(odd == 1, pair, down)

    scatter = Scatter(
        place, windows, number, grads_h, fin_h,
        (grad, got0, out1, got1, out2, got2, mid, out3, got3, out4, got4, fin, squares, load_sem, s_send, s_recv, fin_sem, credit),
    )

    def backward(aT, hid, wdc, dout):
        ps, dg, du = (hid.at[pl.ds(2 * i, 2)] for i in range(3))

        def weights_of(layer, u, slot):
            half_no, group = split(u)
            yield gu_load(at_gu(layer, u), slot)
            for part in range(per_down):
                yield pltpu.make_async_copy(
                    buf_h.at[at_down(layer, half_no * per_down + part), div(group, pairs), aligned(rem(group, pairs) * (per // 2), per // 2)],
                    wdc.at[slot, :, :, pl.ds(part * unit_rows, unit_rows)],
                    wd_sem.at[slot, part],
                )

        def down_store(layer, c, slots=2):
            slot = rem(c, slots)
            half_no, group = split(c)
            for part in range(per_down):
                yield pltpu.make_async_copy(
                    dout.at[slot, :, :, pl.ds(part * unit_rows, unit_rows)],
                    grads_h.at[layer * total + units + half_no * per_down + part, aligned(group * (per // 2), per // 2)],
                    dout_sem.at[slot, part],
                )

        def made_in(layer, c):
            return rem((0 if layer else phase3) + blocks * c + blocks - 1, grad.shape[0])

        def body(layer, c, t, now, before, grads, sums):
            top = layer == layers - 1
            backward_body(
                c, t, now, before, grads, blocks, a, aT, by, byT, acc if top else None, ps if top else None, dg, du,
                gate_up, lambda slot: wdc[slot].reshape(gu, d), grad.at[made_in(layer, c)], dout if top else None, sums,
            )

        first, last = jnp.int32(0), jnp.int32(units)
        for cp in weights_of(1, first, first):
            cp.start()

        @pl.loop(0, tokens // strip)
        def _(t):
            rows = aligned(t * strip, strip)
            h1 = (h[rows].astype(F32) + acc[rows].astype(BF16).astype(F32)).astype(BF16)
            h[rows] = h1
            a1 = normed(h1)
            a[rows] = a1
            aT[:, rows] = a1.astype(F32).T.astype(BF16)

        def clear():
            acc[...] = jnp.zeros_like(acc)

        def ticked1(c, t, work):
            if c is last:
                scatter.around(blocks * c + t, work)
                return

            @pl.when((t == 0) & (after + 2 * c < layers * total + GATHER_DEPTH))
            def _():
                gathers(after + 2 * c, 2)

            scatter.around(blocks * c + t, work)

        backward_loop(units, blocks, last, functools.partial(body, 1), functools.partial(weights_of, 1), functools.partial(down_store, 1), ticked1, clear)

        cp_x = pltpu.make_async_copy(x_h, a, in_sem.at[0])
        cp_x.start()

        def p_loads(i):
            for j in range(2):
                slot = 2 * rem(i, 2) + j
                yield pltpu.make_async_copy(p_h.at[2 * i + j], hid.at[slot], p_sem.at[slot])

        def down_stores(i):
            for j in range(2):
                yield from down_store(0, 2 * i + j, 4)

        for cp in itertools.chain(p_loads(first), weights_of(0, first, first)):
            cp.start()
        scatter.tick(jnp.int32(phase1))
        cp_x.wait()

        @pl.loop(0, tokens // strip)
        def _(t):
            rows = aligned(t * strip, strip)
            back = normed_back(h[rows], acc[rows].astype(BF16).astype(F32))
            by1 = (by[rows].astype(F32) + back.astype(F32)).astype(BF16)
            by[rows] = by1
            byT[:, rows] = by1.astype(F32).T.astype(BF16)
            a0 = normed(a[rows])
            a[rows] = a0
            aT[:, rows] = a0.astype(F32).T.astype(BF16)

        scatter.tick(jnp.int32(phase1 + 1))

        @pl.loop(0, units // 2)
        def _(i):
            for cp in p_loads(i):
                cp.wait()

            @pl.when(2 * i + 2 < units)
            def _():
                for cp in p_loads(i + 1):
                    cp.start()

            @pl.when(i > 1)
            def _():
                for cp in down_stores(i - 2):
                    cp.wait()

            def work(sums):
                pieces = list(sums)
                for j in range(2):
                    slot = 2 * rem(i, 2) + j
                    for r in range(0, d, d // 2):
                        m = pl.ds(r, d // 2)
                        part = dot(byT[m], hid[slot])
                        for piece in pieces[:2]:
                            piece()
                        pieces = pieces[2:]
                        dout[slot, :, :, :, m] = part.T.astype(BF16).reshape(dout.shape[1:4] + (d // 2,))

            scatter.around(phase2 + i, work)
            for cp in down_stores(i):
                cp.start()

        for i in (units // 2 - 2, units // 2 - 1):
            for cp in down_stores(jnp.int32(i)):
                cp.wait()

        backward_loop(
            units, blocks, last, functools.partial(body, 0), functools.partial(weights_of, 0), lambda c: (),
            lambda c, t, work: scatter.around(phase3 + blocks * c + t, work),
        )
    pl.run_scoped(
        backward,
        pltpu.VMEM((d, tokens), BF16),
        pltpu.VMEM((6, tokens, gu), BF16),
        pltpu.VMEM((2, per // 2, 2, LANES, d), BF16),
        pltpu.VMEM((4, per // 2, 2, LANES, d), BF16),
    )

    scatter.at = DRAIN_AT
    scatter.allow(CREDIT)
    scatter.paced = False

    @pl.loop(0, len(DRAIN_AT) - 2)
    def _(i):
        scatter.tick(last_tick + 1 + 2 * i)

    scatter.when(last_tick + DRAIN_AT[7], 7, lambda b, s, began: scatter.store(s, 0).wait())

    so_far = jnp.full(rows1.shape[1:], jnp.sum(squares[...]), F32)
    for i, ((spot, length, other), rows) in enumerate(zip(lines, (rows1, rows2), strict=True)):
        rows[spot] = so_far
        cps = [remote(rows.at[spot], rows.at[spot], sum_send.at[i, j], sum_recv.at[i, spot], other(j)) for j in range(1, length)]
        for cp in cps:
            cp.start()
        for j in range(1, length):
            away = rem(spot + j, length)
            pltpu.make_async_copy(rows.at[away], rows.at[away], sum_recv.at[i, away]).wait()
        for cp in cps:
            cp.wait_send()
        so_far = rows[0]
        for j in range(1, length):
            so_far = so_far + rows[j]
    total_o[...] = so_far


def backward_body(c, t, now, before, grads, blocks, a, aT, by, byT, acc, ps, dg, du, gate_up, down, grad, dout, sums):
    slot = rem(c, 2)
    other = 1 - slot
    tokens, d = a.shape
    tb = tokens // blocks
    part = d // blocks
    fill = []

    def states(i):
        slot_b = where(t == 0, other, slot)
        rows_b = aligned(rem(t + blocks - 1, blocks) * tb + i * (tb // 2), tb // 2)
        wg, wu = gate_up(slot_b)
        acc[rows_b] += dot_t(dg[slot_b, rows_b], wg) + dot_t(du[slot_b, rows_b], wu)

    def weights(i):
        m = aligned(t * part, part)
        if i == 2:
            dout[other, :, :, :, m] = dot(byT[m], ps[other]).T.astype(BF16).reshape(dout.shape[1:4] + (part,))
            return
        rows_g = grad.shape[2] // 2
        chips = part // rows_g // 2
        value = dot(aT[m], (dg, du)[i][other]).astype(BF16)
        grad[aligned(t * chips, chips), :, pl.ds(i * rows_g, rows_g)] = value.reshape(chips, 2, rows_g, -1)

    if before and acc is not None:
        fill += [functools.partial(states, i) for i in range(2)]
    if grads:
        fill += [functools.partial(weights, i) for i in range(3 if ps is not None else 2)]
    if sums is not None:
        fill = [piece for pair in itertools.zip_longest(fill, sums) for piece in pair if piece is not None]
    if not now:
        for piece in fill:
            piece()
        return
    wg, wu = gate_up(slot)
    wd = down(slot)
    gu = wg.shape[1]
    tiles = [(r, col) for r in range(0, tb, SUB_ROWS) for col in range(0, gu, SUB_COLS)]
    done = 0
    for i, (r, col) in enumerate(tiles):
        cols = slice(col, col + SUB_COLS)
        rows = aligned(t * tb + r, SUB_ROWS)
        at = a[rows]
        g_all, up_all = dot(at, wg[:, cols]), dot(at, wu[:, cols])
        dp_all = dot_t(by[rows], wd[cols])
        while done < len(fill) * (i + 1) // len(tiles):
            fill[done]()
            done += 1
        for q in range(0, SUB_ROWS, SLICE):
            g, up, dp = g_all[q : q + SLICE], up_all[q : q + SLICE], dp_all[q : q + SLICE].astype(BF16).astype(F32)
            sig = 1.0 / (1.0 + jnp.exp(-g))
            silu = g * sig
            out = aligned(t * tb + r + q, SLICE)
            if ps is not None:
                ps[slot, out, cols] = (silu * up).astype(BF16)
            du[slot, out, cols] = (dp * silu).astype(BF16)
            dg[slot, out, cols] = (dp * up * (sig + silu * (1.0 - sig))).astype(BF16)


def backward_loop(units, blocks, last, body, weights_of, flush, ticked, first_body_done=None):
    zero = jnp.int32(0)

    def each(c, action, copies):
        for cp in copies(c):
            getattr(cp, action)()

    def weights(c):
        return weights_of(c, rem(c, 2))

    each(zero, "wait", weights)

    @pl.loop(0, blocks)
    def _(t):
        ticked(zero, t, lambda sums: body(zero, t, True, True, False, sums))

        @pl.when(t == 0)
        def _():
            each(jnp.int32(1), "start", weights)
            if first_body_done is not None:
                first_body_done()

    @pl.loop(blocks, units * blocks)
    def _(i):
        c, t = div(i, blocks), rem(i, blocks)
        pl.when(t == 0)(lambda: each(c, "wait", weights))
        ticked(c, t, lambda sums: body(c, t, True, True, True, sums))

        @pl.when(t == 0)
        def _():
            pl.when(c + 1 < units)(lambda: each(c + 1, "start", weights))
            pl.when(c > 1)(lambda: each(c - 2, "wait", flush))

        pl.when(t == blocks - 1)(lambda: each(c - 1, "start", flush))

    body(last, zero, False, True, False, None)

    @pl.loop(0, blocks)
    def _(t):
        ticked(last, t, lambda sums: body(last, t, False, False, True, sums))
        pl.when(t == 0)(lambda: each(last - 2, "wait", flush))

    each(last - 1, "start", flush)
    each(last - 1, "wait", flush)


SCATTER_AT = (0, 1, 3, 6, 8, 10, 12, 13)
DRAIN_AT = (0, 1, 3, 5, 7, 9, 11, 13)
CREDIT = 3


class Scatter:
    def __init__(self, place, windows, number, source, target, refs):
        self.place, self.windows, self.number, self.source, self.target = place, windows, number, source, target
        (self.grad, self.got0, self.out1, self.got1, self.out2, self.got2, self.mid, self.out3, self.got3, self.out4, self.got4,
         self.fin, self.squares, self.load_sem, self.send, self.recv, self.fin_sem, self.credit) = refs
        self.half = self.grad.shape[3] // 2
        self.at, self.paced, self.now = SCATTER_AT, True, None

    def slots(self, tau, stage):
        began = tau - self.at[stage] + 2 * self.grad.shape[0] * self.send.shape[0]
        return rem(began, self.grad.shape[0]), rem(began, self.send.shape[0])

    def bounds(self, tau):
        odd = rem(tau, 2) == 1
        return [
            [[where(odd, *(pair if same else pair[::-1])) for pair in zip(o, e, strict=True)] for e, o in zip(*self.windows, strict=True)]
            for same in (True, False)
        ]

    def here(self, tau, stage):
        if self.now is not tau:
            self.now, self.found, self.limits = tau, {}, self.bounds(tau)
        began = tau - self.at[stage]
        (low0, high0), (low1, high1) = self.limits[self.at[stage] % 2]
        if stage not in self.found:
            self.found[stage] = ((began >= low0) & (began < high0)) | ((began >= low1) & (began < high1))
        return self.found[stage]

    def when(self, tau, stage, body):
        b, s = self.slots(tau, stage)
        began = tau - self.at[stage]
        pl.when(self.here(tau, stage))(lambda: body(b, s, began))

    def which(self, began):
        return self.number(began, rem(began, 2))

    def load(self, b, n):
        return pltpu.make_async_copy(self.source.at[n], self.grad.at[b], self.load_sem.at[b])

    def store(self, s, n):
        return pltpu.make_async_copy(self.fin.at[s], self.target.at[n], self.fin_sem.at[s])

    def copies(self, stage, b, s):
        up_a, down_a, up_b, down_b, partner = self.place.neighbours()
        if stage == 1:
            src = self.grad.at[b, :, 1 - self.place.k]
            return (remote(src, self.got0.at[b], self.send.at[s, 0], self.recv.at[s, 0], partner),)
        out, got, base, up, down = (
            (self.out1, self.got1, 1, up_b, down_b),
            (self.out2, self.got2, 3, up_b, down_b),
            (self.out3, self.got3, 5, up_a, down_a),
            (self.out4, self.got4, 7, up_a, down_a),
        )[stage - 2]
        return tuple(
            remote(out.at[s, i], got.at[s, i], self.send.at[s, base + i], self.recv.at[s, base + i], other)
            for i, other in enumerate((up, down))
        )

    def allow(self, ticks):
        for i in range(len(self.place.neighbours())):
            pl.semaphore_wait(self.credit.at[i], ticks)

    def before(self, tau):
        if self.paced:
            pl.when(tau >= CREDIT)(lambda: self.allow(1))

        def down_only(action):
            def body(b, s, began):
                pl.when(rem(began, 2) == 0)(lambda: action(b, began))

            return body

        self.when(tau, 0, down_only(lambda b, began: self.load(b, self.which(began)).start()))

        def across(b, s, began):
            down_only(lambda b, began: self.load(b, 0).wait())(b, s, began)
            for cp in self.copies(1, b, s):
                cp.start()

        self.when(tau, 1, across)
        for stage in range(2, 7):

            def arrived(b, s, began, stage=stage):
                for cp in self.copies(stage - 1, b, s):
                    cp.wait()

            self.when(tau, stage, arrived)
        self.when(tau, 7, lambda b, s, began: self.store(s, 0).wait())

    def after(self, tau):
        for stage in range(2, 6):

            def go(b, s, began, stage=stage):
                for cp in self.copies(stage, b, s):
                    cp.start()

            self.when(tau, stage, go)
        self.when(tau, 6, lambda b, s, began: self.store(s, self.which(began)).start())
        for other, seen_as in zip(self.place.neighbours(), (1, 0, 3, 2, 4), strict=True) if self.paced else ():
            pl.semaphore_signal(self.credit.at[seen_as], inc=1, device_id={"dp": other}, device_id_type=MESH)

    def sums(self, tau):
        return [functools.partial(getattr(self, f"sum{stage}"), tau) for stage in range(2, 7)]

    def mine(self, b, i, step):
        chip = self.place.at(i, rem(self.place.pb + step, self.place.side))
        return self.grad[b, chip, self.place.k].astype(F32) + self.got0[b, chip].astype(F32)

    def sum2(self, tau):
        b, s = self.slots(tau, 2)
        for i in range(self.place.side):
            total = self.mine(b, i, 2)
            self.out1[s, 0, i] = total[: self.half].astype(BF16)
            self.out1[s, 1, i] = total[self.half :].astype(BF16)

    def add_half(self, out, index, way, total, got):
        half = self.half
        whole, rest = slice(half * way, half * way + half), slice(half * (1 - way), half * (2 - way))
        out[index + (pl.ds(half * way, half),)] = (total[whole] + got.astype(F32)).astype(BF16)
        out[index + (pl.ds(half * (1 - way), half),)] = total[rest].astype(BF16)

    def sum3(self, tau):
        b, s = self.slots(tau, 3)
        for i in range(self.place.side):
            for way, step in ((0, 1), (1, self.place.side - 1)):
                self.add_half(self.out2, (s, way, i), way, self.mine(b, i, step), self.got1[s, way, i])

    def sum4(self, tau):
        b, s = self.slots(tau, 4)
        for i in range(self.place.side):
            self.mid[b, i] = self.mine(b, i, 0) + self.got2[s, 0, i].astype(F32) + self.got2[s, 1, i].astype(F32)
        far = self.mid[b, rem(self.place.pa + 2, self.place.side)]
        self.out3[s, 0] = far[: self.half].astype(BF16)
        self.out3[s, 1] = far[self.half :].astype(BF16)

    def sum5(self, tau):
        b, s = self.slots(tau, 5)
        for way, step in ((0, 1), (1, self.place.side - 1)):
            total = self.mid[b, rem(self.place.pa + step, self.place.side)]
            self.add_half(self.out4, (s, way), way, total, self.got3[s, way])

    def sum6(self, tau):
        b, s = self.slots(tau, 6)
        total = self.mid[b, self.place.pa] + self.got4[s, 0].astype(F32) + self.got4[s, 1].astype(F32)
        result = total.astype(BF16)
        self.fin[s] = result
        here = self.here(tau, 6)
        squared = result.astype(F32) * result.astype(F32)
        self.squares[...] += jnp.where(here, squared, 0.0)

    def tick(self, tau):
        self.before(tau)
        for piece in self.sums(tau):
            piece()
        self.after(tau)

    def around(self, tau, work):
        self.before(tau)
        work(self.sums(tau))
        self.after(tau)


def adamw(w, m, v, g):
    w = w.astype(F32)
    m = 0.9 * m + 0.1 * g
    v = 0.95 * v + 0.05 * g * g
    step = m * lax.rsqrt(v + 1e-8) + 0.1 * w
    return (w - 0.02 * step).astype(BF16), m, v


def update_kernel(count, squares, pair0, pair1, down, *refs):
    ins, outs = refs[:9], refs[9:]
    factor = jnp.minimum(1.0, 0.5 * lax.rsqrt(squares[0:1, 0:1] / count + 1e-30))
    rows_g = ins[0].shape[1]
    some, unit_rows, gu = pair0.shape[1:]

    def update(i, where, g):
        new = adamw(*(ref[where] for ref in ins[i::3]), g.astype(F32) * factor)
        for ref, value in zip(outs[i::3], new, strict=True):
            ref[where] = value

    for p in range(some):
        for i in range(2):
            rows = slice(i * rows_g, (i + 1) * rows_g)
            g = [half[0, p, rows, c : c + LANES] for c in range(0, gu, LANES) for half in (pair0, pair1)]
            update(i, (0, slice(None), pl.ds(p * 2 * gu, 2 * gu)), jnp.concatenate(g, 1))
        update(2, (0, pl.ds(p * unit_rows, unit_rows)), down[0, p])


def solution(mesh):
    n_dev = mesh.shape["dp"]

    def step(x, dy, *arrays):
        weights, m, v = (arrays[i : i + 3] for i in (0, 3, 6))
        x, dy = x[0], dy[0]
        w_gate, w_up, w_down = weights
        layers, rows_g, ff = w_gate.shape
        assert layers == 2
        rows_d, d = w_down.shape[1:]
        tokens = x.shape[0]
        chips = n_dev // 2
        halves = rows_d // LANES
        gu = d
        units, unit_rows = ff // gu, 2 * rows_g
        downs = rows_d // unit_rows
        per = gu // LANES
        total = units + downs
        vmem, dma = pltpu.VMEM, pltpu.SemaphoreType.DMA
        shape = jax.ShapeDtypeStruct
        unit = (chips, 2, unit_rows, gu)
        states = (tokens, d)

        big, small, side = 10, 6, math.isqrt(chips)
        whole = (side, side) + unit[1:]
        half_block, block = (unit_rows // 2, gu), (unit_rows, gu)
        _, _, _, fin, squares = pl.pallas_call(
            functools.partial(step_kernel, n_dev),
            out_shape=(
                shape((layers * total,) + whole, BF16),
                shape((units, tokens, gu), BF16),
                shape((layers * total,) + unit, BF16),
                shape((layers * total,) + block, BF16),
                shape((8, LANES), F32),
            ),
            in_specs=[ANY] * 5,
            out_specs=[ANY] * 4 + [pl.BlockSpec(memory_space=vmem)],
            scratch_shapes=[
                vmem((layers * total,) + block, BF16),
                vmem(states, BF16),
                vmem(states, BF16),
                vmem(states, BF16),
                vmem(states, F32),
                vmem((2,) + whole, BF16),
                vmem(states[::-1], BF16),
                vmem((big,) + unit, BF16),
                vmem((big, chips) + block, BF16),
                vmem((small, 2, side) + half_block, BF16),
                vmem((small, 2, side) + half_block, BF16),
                vmem((small, 2, side) + block, BF16),
                vmem((small, 2, side) + block, BF16),
                vmem((big, side) + block, F32),
                vmem((small, 2) + half_block, BF16),
                vmem((small, 2) + half_block, BF16),
                vmem((small, 2) + block, BF16),
                vmem((small, 2) + block, BF16),
                vmem((small,) + block, BF16),
                vmem(block, F32),
                vmem((2 * side, 8, LANES), F32),
                vmem((side, 8, LANES), F32),
                dma((8,)),
                dma((8, 9)),
                dma((8, 9)),
                dma((4,)),
                dma((2,)),
                dma((2, downs // halves)),
                dma((units // halves,)),
                dma((4, downs // halves)),
                dma((big,)),
                dma((small, 9)),
                dma((small, 9)),
                dma((small,)),
                pltpu.SemaphoreType.REGULAR((5,)),
                dma((2, 2 * side)),
                dma((2, 2 * side)),
            ],
            compiler_params=pltpu.CompilerParams(collective_id=0, has_side_effects=True, vmem_limit_bytes=VMEM_LIMIT),
            name="step",
        )(x, dy, w_gate, w_up, w_down)
        fin = fin.reshape((layers, total) + block)
        some = 2
        steps = units // halves // some
        pair_block, down_block = (1, rows_g, some * halves * gu), (1, some * unit_rows, d)
        fins = [pl.BlockSpec((1, some) + block, lambda i, j, k=k: (i, k * steps + j, 0, 0)) for k in range(3)]
        each = [pl.BlockSpec(pair_block, lambda i, j: (i, 0, j))] * 2 + [pl.BlockSpec(down_block, lambda i, j: (i, j, 0))]
        kinds = [shape(w.shape, t) for t in (BF16, F32, F32) for w in weights]
        elements = layers * total * unit_rows * gu
        return pl.pallas_call(
            functools.partial(update_kernel, n_dev * elements),
            grid=(layers, steps),
            out_shape=kinds,
            in_specs=[pl.BlockSpec(squares.shape, lambda i, j: (0, 0))] + fins + each * 3,
            out_specs=each * 3,
            cost_estimate=pl.CostEstimate(flops=20 * elements, bytes_accessed=22 * elements, transcendentals=elements),
            name="update",
        )(squares, fin, fin, fin, *weights, *m, *v)

    states, cut = P(("rep", "dp"), None, None), P(None, "dp", None)
    return jax.shard_map(
        step,
        mesh=mesh,
        in_specs=(states, states) + (cut,) * 9,
        out_specs=(P("rep", "dp", None),) * 9,
        check_vma=False,
    )
```

```python
import functools
import itertools
import math

import jax
import jax.numpy as jnp
from jax import lax
from jax.experimental import pallas as pl
from jax.experimental.pallas import tpu as pltpu
from jax.sharding import PartitionSpec as P

F32, BF16 = jnp.float32, jnp.bfloat16
MESH = pl.DeviceIdType.MESH
ANY = pl.BlockSpec(memory_space=pl.ANY)
VMEM_LIMIT = 63 * 1024 * 1024
LANES = 128
SUB_ROWS, SUB_COLS, SLICE = 512, 256, 32


def dot(a, b):
    return jnp.dot(a, b, preferred_element_type=F32)


def dot_t(a, b):
    return lax.dot_general(a, b, (((1,), (1,)), ((), ())), preferred_element_type=F32)


def aligned(start, size):
    return pl.ds(pl.multiple_of(start, size), size)


def div(a, b):
    return lax.div(a, jnp.int32(b))


def rem(a, b):
    return lax.rem(a, jnp.int32(b))


def where(test, a, b):
    return lax.select(test, jnp.asarray(a, jnp.int32), jnp.asarray(b, jnp.int32))


def normed(h):
    wide = h.astype(F32)
    return (wide * lax.rsqrt(jnp.mean(wide * wide, -1, keepdims=True) + 1e-6)).astype(BF16)


def normed_back(h, by_a):
    wide = h.astype(F32)
    scale = lax.rsqrt(jnp.mean(wide * wide, -1, keepdims=True) + 1e-6)
    inner = jnp.mean(by_a * wide, -1, keepdims=True)
    return (by_a * scale - wide * (scale * scale * scale * inner)).astype(BF16)


class Place:
    def __init__(self, n):
        self.side = math.isqrt(n // 2)
        assert self.side == 4 and self.side * self.side * 2 == n, n
        self.me = lax.axis_index("dp")
        self.k = rem(self.me, 2)
        chip = div(self.me, 2)
        x, y = div(chip, self.side), rem(chip, self.side)
        self.pa = where(self.k == 0, x, y)
        self.pb = where(self.k == 0, y, x)
        self.partner = chip * 2 + 1 - self.k
        self.x, self.y = x, y
        self.near = self.core(1, 0), self.core(-1, 0), self.core(0, 1), self.core(0, -1), self.partner

    def lines(self):
        side, row = self.side, 2 * self.side
        spot = self.x * 2 + self.k

        def along_x(i):
            i = rem(spot + i, row)
            return (div(i, 2) * side + self.y) * 2 + rem(i, 2)

        def along_y(i):
            return (self.x * side + rem(self.y + i, side)) * 2 + self.k

        return (spot, row, along_x), (self.y, side, along_y)

    def spot(self, a, b):
        a, b = rem(self.pa + a + self.side, self.side), rem(self.pb + b + self.side, self.side)
        return where(self.k == 0, a, b), where(self.k == 0, b, a)

    def chip(self, a, b):
        a, b = rem(self.pa + a + self.side, self.side), rem(self.pb + b + self.side, self.side)
        return self.at(a, b)

    def at(self, a, b):
        return where(self.k == 0, a * self.side + b, b * self.side + a)

    def core(self, a, b):
        return self.chip(a, b) * 2 + self.k

    def neighbours(self):
        return self.near


def greet(others):
    barrier = pltpu.get_barrier_semaphore()
    for other in others:
        pl.semaphore_signal(barrier, inc=1, device_id={"dp": other}, device_id_type=MESH)
    pl.semaphore_wait(barrier, len(others))


def remote(src, dst, send, recv, other):
    return pltpu.make_async_remote_copy(
        src_ref=src, dst_ref=dst, send_sem=send, recv_sem=recv, device_id={"dp": other}, device_id_type=MESH
    )


def gather_tick(place, tau, total, sems, own, buf):
    own_sem, send, recv = sems
    up_a, down_a, up_b, down_b, partner = place.neighbours()
    k = place.k
    half = own.shape[1] // 2
    low, high = pl.ds(0, half), pl.ds(half, half)
    slots = own_sem.shape[0]

    def stage(number, body):
        n = tau - 2 * number
        pl.when((n >= 0) & (n < total))(lambda: body(n, rem(n, slots)))

    def two(n, s, base, src_up, src_down, up, down):
        return (
            remote(src_up, src_up, send.at[s, base], recv.at[s, base], up),
            remote(src_down, src_down, send.at[s, base + 1], recv.at[s, base + 1], down),
        )

    def at(n, a, b, *rows):
        x, y = place.spot(a, b)
        return buf.at[(n, x, y, k) + rows]

    def own_copies(n, s):
        src, dst = own.at[n], at(n, 0, 0)
        return (
            remote(src, dst, send.at[s, 0], recv.at[s, 0], up_a),
            remote(src, dst, send.at[s, 1], recv.at[s, 1], down_a),
        )

    def along_a(n, s):
        return two(n, s, 2, at(n, -1, 0, low), at(n, 1, 0, high), up_a, down_a)

    def lines(n, b, rows=slice(None)):
        x, y = place.spot(0, b)
        yield from (buf.at[n, :, y, 0, rows], buf.at[n, x, :, 1, rows])

    def start_lines(s, base, ups, downs):
        for core, (src_up, src_down) in enumerate(zip(ups, downs, strict=True)):

            @pl.when(k == core)
            def _():
                for cp in two(None, s, base, src_up, src_down, up_b, down_b):
                    cp.start()

    def across(n, s):
        plane = buf.at[n, :, :, k]
        return remote(plane, plane, send.at[s, 8], recv.at[s, 8], partner)

    def wait_both(n, s, base, size):
        for d in range(2):
            for sem in (send, recv):
                pltpu.make_async_copy(size(n), size(n), sem.at[s, base + d]).wait()

    one = lambda n: buf.at[n, 0, 0, 0]
    one_half = lambda n: buf.at[n, 0, 0, 0, low]
    four = lambda n: buf.at[n, 0, :, 0]
    four_half = lambda n: buf.at[n, 0, :, 0, low]

    def stage0(n, s):
        for cp in own_copies(n, s):
            cp.start()
        pltpu.make_async_copy(own.at[n], at(n, 0, 0), own_sem.at[s]).start()

    def stage1(n, s):
        wait_both(n, s, 0, one)
        for cp in along_a(n, s):
            cp.start()
        pltpu.make_async_copy(own.at[n], at(n, 0, 0), own_sem.at[s]).wait()

    def stage2(n, s):
        wait_both(n, s, 2, one_half)
        start_lines(s, 4, lines(n, 0), lines(n, 0))

    def stage3(n, s):
        wait_both(n, s, 4, four)
        start_lines(s, 6, lines(n, -1, low), lines(n, 1, high))

    def stage4(n, s):
        wait_both(n, s, 6, four_half)
        across(n, s).start()

    def stage5(n, s):
        across(n, s).wait()

    for number, body in enumerate((stage0, stage1, stage2, stage3, stage4, stage5)):
        stage(number, body)


GATHER_DEPTH = 10


def step_kernel(
    n_dev, x_h, dy_h, wg_h, wu_h, wd_h,
    buf_h, p_h, grads_h, fin_h, total_o,
    own, h, a, by, acc, guv,
    byT, grad, got0, out1, got1, out2, got2, mid, out3, got3, out4, got4, fin, squares, rows1, rows2,
    own_sem, g_send, g_recv, in_sem, gu_sem, wd_sem, p_sem, dout_sem,
    load_sem, s_send, s_recv, fin_sem, credit, sum_send, sum_recv,
):
    place = Place(n_dev)
    layers, rows_g, ff = wg_h.shape
    rows_d = wd_h.shape[1]
    tokens, d = x_h.shape
    blocks, quarters, strip = 2, 4, 256
    chips = n_dev // 2
    unit_rows, gu = own.shape[1:]
    per = gu // LANES
    units = ff // gu
    downs = rows_d // unit_rows
    halves = rows_d // LANES
    per_half, per_down = units // halves, downs // halves
    unit = (chips, 2, unit_rows, gu)
    pairs = place.side * 2 // per
    assert halves == 2 and units == 2 * downs and layers == 2
    total = units + downs

    def split(u):
        return div(u, per_half), rem(u, per_half)

    def at_gu(layer, u):
        half_no, i = split(u)
        return layer * total + half_no * (per_half + per_down) + (layer * per_down) + i

    def at_down(layer, q):
        half_no, i = div(q, per_down), rem(q, per_down)
        return layer * total + half_no * (per_half + per_down) + ((1 - layer) * per_half) + i

    def own_pieces(layer, u, sem):
        half_no, group = split(u)
        n = at_gu(layer, u)
        for j in range(per):
            cols = aligned((group * per + j) * rows_d + half_no * LANES, LANES)
            for w, r in ((wg_h, 0), (wu_h, rows_g)):
                yield pltpu.make_async_copy(
                    w.at[layer, :, cols], own.at[n, pl.ds(r, rows_g), pl.ds(j * LANES, LANES)], in_sem.at[sem]
                )

    def own_down(layer, q, sem):
        return pltpu.make_async_copy(wd_h.at[layer, aligned(q * unit_rows, unit_rows)], own.at[at_down(layer, q)], in_sem.at[sem])

    early = 4

    @pl.loop(0, early)
    def _(u):
        for cp in own_pieces(0, u, 2):
            cp.start()

    loads = [(x_h, h), (dy_h, by)]
    for i, (src, dst) in enumerate(loads):
        pltpu.make_async_copy(src, dst, in_sem.at[i]).start()

    lines = place.lines()
    greet([other(i) for _, length, other in lines for i in range(1, length)])
    pltpu.make_async_copy(own.at[pl.ds(0, early)], own.at[pl.ds(0, early)], in_sem.at[2]).wait()

    def gather(tau):
        gather_tick(place, tau, layers * total, (own_sem, g_send, g_recv), own, buf_h)

    def gathers(first, count):
        @pl.loop(0, count)
        def _(i):
            gather(first + i)

    gathers(0, 2)

    def own_loads(layer, start):
        @pl.loop(start, units)
        def _(u):
            for cp in own_pieces(layer, u, 3 - layer):
                cp.start()

        @pl.loop(0, downs)
        def _(q):
            own_down(layer, q, 3 - layer).start()

    own_loads(0, early)
    for i, (src, dst) in enumerate(loads):
        pltpu.make_async_copy(src, dst, in_sem.at[i]).wait()

    @pl.loop(0, tokens // strip)
    def _(t):
        rows = aligned(t * strip, strip)
        a[rows] = normed(h[rows])
        acc[rows] = jnp.zeros((strip, d), F32)

    squares[...] = jnp.zeros_like(squares)
    rest = own.at[pl.ds(early, total - early)]
    pltpu.make_async_copy(rest, rest, in_sem.at[3]).wait()
    own_loads(1, 0)
    strips = tokens // strip

    def gu_load(n, slot):
        return pltpu.make_async_copy(buf_h.at[n], guv.at[slot], gu_sem.at[slot])

    def gate_up(slot):
        w = guv[slot].reshape(n_dev, unit_rows, gu)
        return w[:, :rows_g].reshape(d, gu), w[:, rows_g:].reshape(d, gu)

    def forward(pbuf, wdv):
        slots = pbuf.shape[0]

        def wd_load(q):
            part = rem(q, per_down)
            return pltpu.make_async_copy(
                buf_h.at[at_down(0, q)], wdv.at[:, :, :, aligned(part * unit_rows, unit_rows)], wd_sem.at[0, part]
            )

        def p_store(u):
            slot = rem(u, slots)
            return pltpu.make_async_copy(pbuf.at[slot], p_h.at[u], p_sem.at[slot])

        def hidden(u):
            slot, out = rem(u, 2), rem(u, slots)
            gu_load(at_gu(0, u), slot).wait()
            pl.when(u >= slots)(lambda: p_store(u - slots).wait())

            @pl.loop(0, blocks)
            def _(t):
                tb = tokens // blocks
                wg, wu = gate_up(slot)
                for r in range(0, tb, SUB_ROWS):
                    at = a[aligned(t * tb + r, SUB_ROWS)]
                    for col in range(0, gu, SUB_COLS):
                        cols = slice(col, col + SUB_COLS)
                        g_all, up_all = dot(at, wg[:, cols]), dot(at, wu[:, cols])
                        for q in range(0, SUB_ROWS, SLICE):
                            g, up = g_all[q : q + SLICE], up_all[q : q + SLICE]
                            hid = g * (1.0 / (1.0 + jnp.exp(-g))) * up
                            pbuf[out, aligned(t * tb + r + q, SLICE), cols] = hid.astype(BF16)

            p_store(u).start()

        @pl.loop(2, GATHER_DEPTH + 1)
        def _(tau):
            gather(tau)
            pl.when(tau == GATHER_DEPTH)(lambda: gu_load(0, 0).start())

            @pl.when(tau < 2 + strips)
            def _():
                rows = aligned((tau - 2) * strip, strip)
                byT[:, rows] = by[rows].astype(F32).T.astype(BF16)

        rest = own.at[pl.ds(total, total)]
        pltpu.make_async_copy(rest, rest, in_sem.at[2]).wait()

        @pl.loop(0, halves)
        def _(half_no):
            now = GATHER_DEPTH + 1 + half_no * (per_half + per_down - 1 + quarters)

            @pl.loop(0, per_half)
            def _(i):
                gather(now + i)
                u = half_no * per_half + i

                @pl.when(i + 1 < per_half)
                def _():
                    gu_load(at_gu(0, u + 1), rem(u + 1, 2)).start()

                q = i - per_half + per_down

                @pl.when((q >= 0) & (half_no == 1))
                def _():
                    wd_load(per_down + q).start()

                hidden(u)

            now += per_half

            @pl.when(half_no == 0)
            def _():
                @pl.loop(0, per_down)
                def _(q):
                    pl.when(q > 0)(lambda: gather(now + q - 1))
                    wd_load(q).start()

            now += where(half_no == 0, per_down - 1, 0)
            for q in range(per_down):
                wd_load(jnp.int32(q)).wait()

            @pl.loop(0, quarters)
            def _(t):
                gather(now + t)

                @pl.when((t == quarters - 1) & (half_no == 0))
                def _():
                    gu_load(at_gu(0, per_half), 0).start()

                rows = aligned(t * (tokens // quarters), tokens // quarters)
                result = acc[rows]
                for j in range(per_half):
                    w = wdv[j // pairs, pl.ds(j % pairs * (per // 2), per // 2)].reshape(gu, d)
                    result += dot(pbuf[j, rows], w)
                acc[rows] = result

        for i in range(slots):
            p_store(jnp.int32(units - slots + i)).wait()

    pl.run_scoped(
        forward,
        pltpu.VMEM((per_half, tokens, gu), BF16),
        pltpu.VMEM((place.side, place.side, 2, LANES, d), BF16),
    )
    after = GATHER_DEPTH + 1 + per_half + (per_down - 1) + quarters + per_half + quarters

    gathers(after, 2)
    after += 2

    phase1 = blocks * (units + 1)
    phase2 = phase1 + 2
    phase3 = phase2 + units // 2
    made = 2 * blocks - 1
    early_down = blocks * (per_half + 2)
    later = downs - per_down
    last_tick = phase3 + made + 2 * (units - 1)
    windows = (
        ((early_down, early_down + 2 * per_down), (phase2, phase3 + 2 * downs)),
        ((made, made + 2 * units), (phase3 + made, last_tick + 2)),
    )
    assert blocks == 2 and phase3 == phase2 + 2 * later and phase3 % 2 == 0 and early_down % 2 == 0 and made % 2 == 1

    assert last_tick == phase3 + blocks * (units + 1) - 1

    def number(tau, odd):
        pair = where(tau < phase2, total + div(tau - made, 2), div(tau - phase3 - made, 2))
        down = where(tau < phase3, total + units + per_down + div(tau - phase2, 2), units + div(tau - phase3, 2))
        down = where(tau < phase2, total + units + div(tau - early_down, 2), down)
        return where(odd == 1, pair, down)

    scatter = Scatter(
        place, windows, number, grads_h, fin_h,
        (grad, got0, out1, got1, out2, got2, mid, out3, got3, out4, got4, fin, squares, load_sem, s_send, s_recv, fin_sem, credit),
    )

    def backward(aT, hid, wdc, dout):
        ps, dg, du = (hid.at[pl.ds(2 * i, 2)] for i in range(3))

        def weights_of(layer, u, slot):
            half_no, group = split(u)
            yield gu_load(at_gu(layer, u), slot)
            for part in range(per_down):
                yield pltpu.make_async_copy(
                    buf_h.at[at_down(layer, half_no * per_down + part), div(group, pairs), aligned(rem(group, pairs) * (per // 2), per // 2)],
                    wdc.at[slot, :, :, pl.ds(part * unit_rows, unit_rows)],
                    wd_sem.at[slot, part],
                )

        def down_store(layer, c, slots=2):
            slot = rem(c, slots)
            half_no, group = split(c)
            for part in range(per_down):
                yield pltpu.make_async_copy(
                    dout.at[slot, :, :, pl.ds(part * unit_rows, unit_rows)],
                    grads_h.at[layer * total + units + half_no * per_down + part, aligned(group * (per // 2), per // 2)],
                    dout_sem.at[slot, part],
                )

        def made_in(layer, c):
            return rem((0 if layer else phase3) + blocks * c + blocks - 1, grad.shape[0])

        def body(layer, c, t, now, before, grads, sums):
            top = layer == layers - 1
            backward_body(
                c, t, now, before, grads, blocks, a, aT, by, byT, acc if top else None, ps if top else None, dg, du,
                gate_up, lambda slot: wdc[slot].reshape(gu, d), grad.at[made_in(layer, c)], dout if top else None, sums,
            )

        first, last = jnp.int32(0), jnp.int32(units)
        for cp in weights_of(1, first, first):
            cp.start()

        @pl.loop(0, tokens // strip)
        def _(t):
            rows = aligned(t * strip, strip)
            h1 = (h[rows].astype(F32) + acc[rows].astype(BF16).astype(F32)).astype(BF16)
            h[rows] = h1
            a1 = normed(h1)
            a[rows] = a1
            aT[:, rows] = a1.astype(F32).T.astype(BF16)

        def clear():
            acc[...] = jnp.zeros_like(acc)

        def ticked1(c, t, work):
            if c is last:
                scatter.around(blocks * c + t, work)
                return

            @pl.when((t == 0) & (after + 2 * c < layers * total + GATHER_DEPTH))
            def _():
                gathers(after + 2 * c, 2)

            scatter.around(blocks * c + t, work)

        backward_loop(units, blocks, last, functools.partial(body, 1), functools.partial(weights_of, 1), functools.partial(down_store, 1), ticked1, clear)

        cp_x = pltpu.make_async_copy(x_h, a, in_sem.at[0])
        cp_x.start()

        def p_loads(i):
            for j in range(2):
                slot = 2 * rem(i, 2) + j
                yield pltpu.make_async_copy(p_h.at[2 * i + j], hid.at[slot], p_sem.at[slot])

        def down_stores(i):
            for j in range(2):
                yield from down_store(0, 2 * i + j, 4)

        for cp in itertools.chain(p_loads(first), weights_of(0, first, first)):
            cp.start()
        scatter.tick(jnp.int32(phase1))
        cp_x.wait()

        @pl.loop(0, tokens // strip)
        def _(t):
            rows = aligned(t * strip, strip)
            back = normed_back(h[rows], acc[rows].astype(BF16).astype(F32))
            by1 = (by[rows].astype(F32) + back.astype(F32)).astype(BF16)
            by[rows] = by1
            byT[:, rows] = by1.astype(F32).T.astype(BF16)
            a0 = normed(a[rows])
            a[rows] = a0
            aT[:, rows] = a0.astype(F32).T.astype(BF16)

        scatter.tick(jnp.int32(phase1 + 1))

        @pl.loop(0, units // 2)
        def _(i):
            for cp in p_loads(i):
                cp.wait()

            @pl.when(2 * i + 2 < units)
            def _():
                for cp in p_loads(i + 1):
                    cp.start()

            @pl.when(i > 1)
            def _():
                for cp in down_stores(i - 2):
                    cp.wait()

            def work(sums):
                pieces = list(sums)
                for j in range(2):
                    slot = 2 * rem(i, 2) + j
                    for r in range(0, d, d // 2):
                        m = pl.ds(r, d // 2)
                        part = dot(byT[m], hid[slot])
                        for piece in pieces[:2]:
                            piece()
                        pieces = pieces[2:]
                        dout[slot, :, :, :, m] = part.T.astype(BF16).reshape(dout.shape[1:4] + (d // 2,))

            scatter.around(phase2 + i, work)
            for cp in down_stores(i):
                cp.start()

        for i in (units // 2 - 2, units // 2 - 1):
            for cp in down_stores(jnp.int32(i)):
                cp.wait()

        backward_loop(
            units, blocks, last, functools.partial(body, 0), functools.partial(weights_of, 0), lambda c: (),
            lambda c, t, work: scatter.around(phase3 + blocks * c + t, work),
        )
    pl.run_scoped(
        backward,
        pltpu.VMEM((d, tokens), BF16),
        pltpu.VMEM((6, tokens, gu), BF16),
        pltpu.VMEM((2, per // 2, 2, LANES, d), BF16),
        pltpu.VMEM((4, per // 2, 2, LANES, d), BF16),
    )

    scatter.allow(CREDIT)
    scatter.paced = False

    @pl.loop(0, SCATTER_AT[-1])
    def _(i):
        scatter.tick(last_tick + 1 + i)

    so_far = jnp.full(rows1.shape[1:], jnp.sum(squares[...]), F32)
    for i, ((spot, length, other), rows) in enumerate(zip(lines, (rows1, rows2), strict=True)):
        rows[spot] = so_far
        cps = [remote(rows.at[spot], rows.at[spot], sum_send.at[i, j], sum_recv.at[i, spot], other(j)) for j in range(1, length)]
        for cp in cps:
            cp.start()
        for j in range(1, length):
            away = rem(spot + j, length)
            pltpu.make_async_copy(rows.at[away], rows.at[away], sum_recv.at[i, away]).wait()
        for cp in cps:
            cp.wait_send()
        so_far = rows[0]
        for j in range(1, length):
            so_far = so_far + rows[j]
    total_o[...] = so_far


def backward_body(c, t, now, before, grads, blocks, a, aT, by, byT, acc, ps, dg, du, gate_up, down, grad, dout, sums):
    slot = rem(c, 2)
    other = 1 - slot
    tokens, d = a.shape
    tb = tokens // blocks
    part = d // blocks
    fill = []

    def states(i):
        slot_b = where(t == 0, other, slot)
        rows_b = aligned(rem(t + blocks - 1, blocks) * tb + i * (tb // 2), tb // 2)
        wg, wu = gate_up(slot_b)
        acc[rows_b] += dot_t(dg[slot_b, rows_b], wg) + dot_t(du[slot_b, rows_b], wu)

    def weights(i):
        m = aligned(t * part, part)
        if i == 2:
            dout[other, :, :, :, m] = dot(byT[m], ps[other]).T.astype(BF16).reshape(dout.shape[1:4] + (part,))
            return
        rows_g = grad.shape[2] // 2
        chips = part // rows_g // 2
        value = dot(aT[m], (dg, du)[i][other]).astype(BF16)
        grad[aligned(t * chips, chips), :, pl.ds(i * rows_g, rows_g)] = value.reshape(chips, 2, rows_g, -1)

    if before and acc is not None:
        fill += [functools.partial(states, i) for i in range(2)]
    if grads:
        fill += [functools.partial(weights, i) for i in range(3 if ps is not None else 2)]
    if sums is not None:
        fill = [piece for pair in itertools.zip_longest(sums, fill) for piece in pair if piece is not None]
    if not now:
        for piece in fill:
            piece()
        return
    wg, wu = gate_up(slot)
    wd = down(slot)
    gu = wg.shape[1]
    tiles = [(r, col) for r in range(0, tb, SUB_ROWS) for col in range(0, gu, SUB_COLS)]
    done = 0
    for i, (r, col) in enumerate(tiles):
        cols = slice(col, col + SUB_COLS)
        rows = aligned(t * tb + r, SUB_ROWS)
        at = a[rows]
        g_all, up_all = dot(at, wg[:, cols]), dot(at, wu[:, cols])
        dp_all = dot_t(by[rows], wd[cols])
        while done < len(fill) * (i + 1) // len(tiles):
            fill[done]()
            done += 1
        for q in range(0, SUB_ROWS, SLICE):
            g, up, dp = g_all[q : q + SLICE], up_all[q : q + SLICE], dp_all[q : q + SLICE].astype(BF16).astype(F32)
            sig = 1.0 / (1.0 + jnp.exp(-g))
            silu = g * sig
            out = aligned(t * tb + r + q, SLICE)
            if ps is not None:
                ps[slot, out, cols] = (silu * up).astype(BF16)
            du[slot, out, cols] = (dp * silu).astype(BF16)
            dg[slot, out, cols] = (dp * up * (sig + silu * (1.0 - sig))).astype(BF16)


def backward_loop(units, blocks, last, body, weights_of, flush, ticked, first_body_done=None):
    zero = jnp.int32(0)

    def each(c, action, copies):
        for cp in copies(c):
            getattr(cp, action)()

    def weights(c):
        return weights_of(c, rem(c, 2))

    each(zero, "wait", weights)

    @pl.loop(0, blocks)
    def _(t):
        ticked(zero, t, lambda sums: body(zero, t, True, True, False, sums))

        @pl.when(t == 0)
        def _():
            each(jnp.int32(1), "start", weights)
            if first_body_done is not None:
                first_body_done()

    @pl.loop(blocks, units * blocks)
    def _(i):
        c, t = div(i, blocks), rem(i, blocks)
        pl.when(t == 0)(lambda: each(c, "wait", weights))
        ticked(c, t, lambda sums: body(c, t, True, True, True, sums))

        @pl.when(t == 0)
        def _():
            pl.when(c + 1 < units)(lambda: each(c + 1, "start", weights))
            pl.when(c > 1)(lambda: each(c - 2, "wait", flush))

        pl.when(t == blocks - 1)(lambda: each(c - 1, "start", flush))

    body(last, zero, False, True, False, None)

    @pl.loop(0, blocks)
    def _(t):
        ticked(last, t, lambda sums: body(last, t, False, False, True, sums))
        pl.when(t == 0)(lambda: each(last - 2, "wait", flush))

    each(last - 1, "start", flush)
    each(last - 1, "wait", flush)


SCATTER_AT = (0, 1, 3, 6, 9, 11, 13, 14)
CREDIT = 2


class Scatter:
    def __init__(self, place, windows, number, source, target, refs):
        self.place, self.windows, self.number, self.source, self.target = place, windows, number, source, target
        (self.grad, self.got0, self.out1, self.got1, self.out2, self.got2, self.mid, self.out3, self.got3, self.out4, self.got4,
         self.fin, self.squares, self.load_sem, self.send, self.recv, self.fin_sem, self.credit) = refs
        self.half = self.grad.shape[3] // 2
        self.at, self.paced, self.now = SCATTER_AT, True, None

    def slots(self, tau, stage):
        began = tau - self.at[stage] + 2 * self.grad.shape[0] * self.send.shape[0]
        return rem(began, self.grad.shape[0]), rem(began, self.send.shape[0])

    def bounds(self, tau):
        odd = rem(tau, 2) == 1
        return [
            [[where(odd, *(pair if same else pair[::-1])) for pair in zip(o, e, strict=True)] for e, o in zip(*self.windows, strict=True)]
            for same in (True, False)
        ]

    def here(self, tau, stage):
        if self.now is not tau:
            self.now, self.found, self.limits = tau, {}, self.bounds(tau)
        began = tau - self.at[stage]
        (low0, high0), (low1, high1) = self.limits[self.at[stage] % 2]
        if stage not in self.found:
            self.found[stage] = ((began >= low0) & (began < high0)) | ((began >= low1) & (began < high1))
        return self.found[stage]

    def when(self, tau, stage, body):
        b, s = self.slots(tau, stage)
        began = tau - self.at[stage]
        pl.when(self.here(tau, stage))(lambda: body(b, s, began))

    def which(self, began):
        return self.number(began, rem(began, 2))

    def load(self, b, n):
        return pltpu.make_async_copy(self.source.at[n], self.grad.at[b], self.load_sem.at[b])

    def store(self, s, n):
        return pltpu.make_async_copy(self.fin.at[s], self.target.at[n], self.fin_sem.at[s])

    def copies(self, stage, b, s):
        up_a, down_a, up_b, down_b, partner = self.place.neighbours()
        if stage == 1:
            src = self.grad.at[b, :, 1 - self.place.k]
            return (remote(src, self.got0.at[b], self.send.at[s, 0], self.recv.at[s, 0], partner),)
        out, got, base, up, down = (
            (self.out1, self.got1, 1, up_b, down_b),
            (self.out2, self.got2, 3, up_b, down_b),
            (self.out3, self.got3, 5, up_a, down_a),
            (self.out4, self.got4, 7, up_a, down_a),
        )[stage - 2]
        return tuple(
            remote(out.at[s, i], got.at[s, i], self.send.at[s, base + i], self.recv.at[s, base + i], other)
            for i, other in enumerate((up, down))
        )

    def allow(self, ticks):
        for i in range(len(self.place.neighbours())):
            pl.semaphore_wait(self.credit.at[i], ticks)

    def before(self, tau):
        if self.paced:
            pl.when(tau >= CREDIT)(lambda: self.allow(1))

        def down_only(action):
            def body(b, s, began):
                pl.when(rem(began, 2) == 0)(lambda: action(b, began))

            return body

        self.when(tau, 0, down_only(lambda b, began: self.load(b, self.which(began)).start()))

        def across(b, s, began):
            down_only(lambda b, began: self.load(b, 0).wait())(b, s, began)
            for cp in self.copies(1, b, s):
                cp.start()

        self.when(tau, 1, across)
        for stage in range(2, 7):

            def arrived(b, s, began, stage=stage):
                for cp in self.copies(stage - 1, b, s):
                    cp.wait()

            self.when(tau, stage, arrived)
        self.when(tau, 7, lambda b, s, began: self.store(s, 0).wait())

    def after(self, tau):
        for stage in range(2, 6):

            def go(b, s, began, stage=stage):
                for cp in self.copies(stage, b, s):
                    cp.start()

            self.when(tau, stage, go)
        self.when(tau, 6, lambda b, s, began: self.store(s, self.which(began)).start())
        for other, seen_as in zip(self.place.neighbours(), (1, 0, 3, 2, 4), strict=True) if self.paced else ():
            pl.semaphore_signal(self.credit.at[seen_as], inc=1, device_id={"dp": other}, device_id_type=MESH)

    def sums(self, tau):
        return [functools.partial(getattr(self, f"sum{stage}"), tau) for stage in (4, 2, 3, 5, 6)]

    def mine(self, b, i, step):
        chip = self.place.at(i, rem(self.place.pb + step, self.place.side))
        return self.grad[b, chip, self.place.k].astype(F32) + self.got0[b, chip].astype(F32)

    def sum2(self, tau):
        b, s = self.slots(tau, 2)
        for i in range(self.place.side):
            total = self.mine(b, i, 2)
            self.out1[s, 0, i] = total[: self.half].astype(BF16)
            self.out1[s, 1, i] = total[self.half :].astype(BF16)

    def add_half(self, out, index, way, total, got):
        half = self.half
        whole, rest = slice(half * way, half * way + half), slice(half * (1 - way), half * (2 - way))
        out[index + (pl.ds(half * way, half),)] = (total[whole] + got.astype(F32)).astype(BF16)
        out[index + (pl.ds(half * (1 - way), half),)] = total[rest].astype(BF16)

    def sum3(self, tau):
        b, s = self.slots(tau, 3)
        for i in range(self.place.side):
            for way, step in ((0, 1), (1, self.place.side - 1)):
                self.add_half(self.out2, (s, way, i), way, self.mine(b, i, step), self.got1[s, way, i])

    def sum4(self, tau):
        b, s = self.slots(tau, 4)
        for i in range(self.place.side):
            self.mid[b, i] = self.mine(b, i, 0) + self.got2[s, 0, i].astype(F32) + self.got2[s, 1, i].astype(F32)
        far = self.mid[b, rem(self.place.pa + 2, self.place.side)]
        self.out3[s, 0] = far[: self.half].astype(BF16)
        self.out3[s, 1] = far[self.half :].astype(BF16)

    def sum5(self, tau):
        b, s = self.slots(tau, 5)
        for way, step in ((0, 1), (1, self.place.side - 1)):
            total = self.mid[b, rem(self.place.pa + step, self.place.side)]
            self.add_half(self.out4, (s, way), way, total, self.got3[s, way])

    def sum6(self, tau):
        b, s = self.slots(tau, 6)
        total = self.mid[b, self.place.pa] + self.got4[s, 0].astype(F32) + self.got4[s, 1].astype(F32)
        result = total.astype(BF16)
        self.fin[s] = result
        here = self.here(tau, 6)
        squared = result.astype(F32) * result.astype(F32)
        self.squares[...] += jnp.where(here, squared, 0.0)

    def tick(self, tau):
        self.before(tau)
        for piece in self.sums(tau):
            piece()
        self.after(tau)

    def around(self, tau, work):
        self.before(tau)
        work(self.sums(tau))
        self.after(tau)


def adamw(w, m, v, g):
    w = w.astype(F32)
    m = 0.9 * m + 0.1 * g
    v = 0.95 * v + 0.05 * g * g
    step = m * lax.rsqrt(v + 1e-8) + 0.1 * w
    return (w - 0.02 * step).astype(BF16), m, v


def update_kernel(count, squares, pair0, pair1, down, *refs):
    ins, outs = refs[:9], refs[9:]
    factor = jnp.minimum(1.0, 0.5 * lax.rsqrt(squares[0:1, 0:1] / count + 1e-30))
    rows_g = ins[0].shape[1]
    some, unit_rows, gu = pair0.shape[1:]

    def update(i, where, g):
        new = adamw(*(ref[where] for ref in ins[i::3]), g.astype(F32) * factor)
        for ref, value in zip(outs[i::3], new, strict=True):
            ref[where] = value

    for p in range(some):
        for i in range(2):
            rows = slice(i * rows_g, (i + 1) * rows_g)
            g = [half[0, p, rows, c : c + LANES] for c in range(0, gu, LANES) for half in (pair0, pair1)]
            update(i, (0, slice(None), pl.ds(p * 2 * gu, 2 * gu)), jnp.concatenate(g, 1))
        update(2, (0, pl.ds(p * unit_rows, unit_rows)), down[0, p])


def solution(mesh):
    n_dev = mesh.shape["dp"]

    def step(x, dy, *arrays):
        weights, m, v = (arrays[i : i + 3] for i in (0, 3, 6))
        x, dy = x[0], dy[0]
        w_gate, w_up, w_down = weights
        layers, rows_g, ff = w_gate.shape
        assert layers == 2
        rows_d, d = w_down.shape[1:]
        tokens = x.shape[0]
        chips = n_dev // 2
        halves = rows_d // LANES
        gu = d
        units, unit_rows = ff // gu, 2 * rows_g
        downs = rows_d // unit_rows
        per = gu // LANES
        total = units + downs
        vmem, dma = pltpu.VMEM, pltpu.SemaphoreType.DMA
        shape = jax.ShapeDtypeStruct
        unit = (chips, 2, unit_rows, gu)
        states = (tokens, d)

        big, small, side = 10, 6, math.isqrt(chips)
        whole = (side, side) + unit[1:]
        half_block, block = (unit_rows // 2, gu), (unit_rows, gu)
        _, _, _, fin, squares = pl.pallas_call(
            functools.partial(step_kernel, n_dev),
            out_shape=(
                shape((layers * total,) + whole, BF16),
                shape((units, tokens, gu), BF16),
                shape((layers * total,) + unit, BF16),
                shape((layers * total,) + block, BF16),
                shape((8, LANES), F32),
            ),
            in_specs=[ANY] * 5,
            out_specs=[ANY] * 4 + [pl.BlockSpec(memory_space=vmem)],
            scratch_shapes=[
                vmem((layers * total,) + block, BF16),
                vmem(states, BF16),
                vmem(states, BF16),
                vmem(states, BF16),
                vmem(states, F32),
                vmem((2,) + whole, BF16),
                vmem(states[::-1], BF16),
                vmem((big,) + unit, BF16),
                vmem((big, chips) + block, BF16),
                vmem((small, 2, side) + half_block, BF16),
                vmem((small, 2, side) + half_block, BF16),
                vmem((small, 2, side) + block, BF16),
                vmem((small, 2, side) + block, BF16),
                vmem((big, side) + block, F32),
                vmem((small, 2) + half_block, BF16),
                vmem((small, 2) + half_block, BF16),
                vmem((small, 2) + block, BF16),
                vmem((small, 2) + block, BF16),
                vmem((small,) + block, BF16),
                vmem(block, F32),
                vmem((2 * side, 8, LANES), F32),
                vmem((side, 8, LANES), F32),
                dma((8,)),
                dma((8, 9)),
                dma((8, 9)),
                dma((4,)),
                dma((2,)),
                dma((2, downs // halves)),
                dma((units // halves,)),
                dma((4, downs // halves)),
                dma((big,)),
                dma((small, 9)),
                dma((small, 9)),
                dma((small,)),
                pltpu.SemaphoreType.REGULAR((5,)),
                dma((2, 2 * side)),
                dma((2, 2 * side)),
            ],
            compiler_params=pltpu.CompilerParams(collective_id=0, has_side_effects=True, vmem_limit_bytes=VMEM_LIMIT),
            name="step",
        )(x, dy, w_gate, w_up, w_down)
        fin = fin.reshape((layers, total) + block)
        some = 2
        steps = units // halves // some
        pair_block, down_block = (1, rows_g, some * halves * gu), (1, some * unit_rows, d)
        fins = [pl.BlockSpec((1, some) + block, lambda i, j, k=k: (i, k * steps + j, 0, 0)) for k in range(3)]
        each = [pl.BlockSpec(pair_block, lambda i, j: (i, 0, j))] * 2 + [pl.BlockSpec(down_block, lambda i, j: (i, j, 0))]
        kinds = [shape(w.shape, t) for t in (BF16, F32, F32) for w in weights]
        elements = layers * total * unit_rows * gu
        return pl.pallas_call(
            functools.partial(update_kernel, n_dev * elements),
            grid=(layers, steps),
            out_shape=kinds,
            in_specs=[pl.BlockSpec(squares.shape, lambda i, j: (0, 0))] + fins + each * 3,
            out_specs=each * 3,
            cost_estimate=pl.CostEstimate(flops=20 * elements, bytes_accessed=22 * elements, transcendentals=elements),
            name="update",
        )(squares, fin, fin, fin, *weights, *m, *v)

    states, cut = P(("rep", "dp"), None, None), P(None, "dp", None)
    return jax.shard_map(
        step,
        mesh=mesh,
        in_specs=(states, states) + (cut,) * 9,
        out_specs=(P("rep", "dp", None),) * 9,
        check_vma=False,
    )
```
